16 devices in a mesh: dp: 4 (over z, y), tp: 4 (over x, core).
Axes of the slice: x: 2, y: 2, z: 2, core: 2. Of those that a mesh axis runs over, the one named last changes fastest.
Arguments:
- x: bfloat16 [2048, 2048], P('dp'), parts along dimension 0
- k_cache: bfloat16 [2048, 16, 16, 128], P('dp', None, 'tp'), parts along dimension 0
- v_cache: bfloat16 [2048, 16, 16, 128], P('dp', None, 'tp'), parts along dimension 0
- positions: int32 [2048], P('dp'), parts along dimension 0
- att_ids: int32 [2048, 2], P('dp'), parts along dimension 0
- mlp_ids: int32 [2048, 2], P('dp'), parts along dimension 0
- norm_att: float32 [2048], replicated
- w_kv: bfloat16 [2048, 16, 256], P(None, 'tp')
- router_att: bfloat16 [2048, 8], replicated
- w_query: bfloat16 [8, 2048, 2048], P(None, None, 'tp')
- w_out: bfloat16 [8, 2048, 2048], P(None, 'tp')
- norm_mlp: float32 [2048], replicated
- router_mlp: bfloat16 [2048, 8], replicated
- w_gate: bfloat16 [8, 2048, 5632], P('tp')
- w_up: bfloat16 [8, 2048, 5632], P('tp')
- w_down: bfloat16 [8, 5632, 2048], P('tp')
Outputs:
- output 1: bfloat16 [2048, 2048], P('dp'), parts along dimension 0
- output 2: bfloat16 [2048, 16, 16, 128], P('dp', None, 'tp'), parts along dimension 0
- output 3: bfloat16 [2048, 16, 16, 128], P('dp', None, 'tp'), parts along dimension 0
There are 4 independent parts. The reference program is written for one: setup_inputs(seed, part) draws one part's arguments, and reference() takes and returns one part's arrays. A program takes and returns all parts, laid end to end along the dimension named above; an argument that names none is the same for every part.
All inputs are finite; a program needn't handle non-finite values.
Results may differ from the reference program's by a relative error of at most 0.0123415.
Values are sent between devices in bfloat16 or wider.
A program may use at most 1 GiB of HBM per device.

```python
import jax
import jax.numpy as jnp
from jax import lax

HIDDEN = 2048
KV_HEADS = 16
HEAD_DIM = 128
ATT_EXPERTS = 8
MLP_EXPERTS = 8
FFN_WIDTH = 5632
TOKENS = 512
CACHE_LEN = 16

QUERY_WIDTH = KV_HEADS * HEAD_DIM
NORM_EPS = 1e-6
ROPE_BASE = 10000.0


def draw_pair(base_key, experts, skewed):
    key_first, key_offset, key_hot, key_share, key_coin = jax.random.split(base_key, 5)
    first_pick = jax.random.randint(key_first, (TOKENS,), 0, experts)
    if skewed:
        hot_id = jax.random.randint(key_hot, (), 0, experts)
        hot_share = jax.random.randint(key_share, (), 40, 61)
        coin_flip = jax.random.randint(key_coin, (TOKENS,), 0, 100)
        first_pick = jnp.where(coin_flip < hot_share, hot_id, first_pick)
    offset = jax.random.randint(key_offset, (TOKENS,), 1, experts)
    token_index = jnp.arange(TOKENS)
    forced = (token_index < experts) & (token_index != first_pick)
    second_pick = jnp.where(forced, token_index, (first_pick + offset) % experts)
    return jnp.stack([first_pick, second_pick], axis=1).astype(jnp.int32)


def draw_positions(base_key):
    positions = jax.random.randint(base_key, (TOKENS,), CACHE_LEN // 4, CACHE_LEN)
    return positions.at[0].set(CACHE_LEN - 1).at[1].set(CACHE_LEN // 4).astype(jnp.int32)


def setup_inputs(seed: int = 0, part: int = 0) -> dict:
    shared_keys = jax.random.split(jax.random.key(seed), 10)
    part_keys = jax.random.split(jax.random.fold_in(jax.random.key(seed + 1), part), 6)
    cache_shape = (TOKENS, CACHE_LEN, KV_HEADS, HEAD_DIM)
    x = jax.random.normal(part_keys[0], (TOKENS, HIDDEN), jnp.float32).astype(jnp.bfloat16)
    k_cache = jax.random.normal(part_keys[1], cache_shape, jnp.float32).astype(jnp.bfloat16)
    value_mean = jax.random.normal(part_keys[2], (TOKENS, 1, KV_HEADS, HEAD_DIM), jnp.float32)
    value_noise = jax.random.normal(part_keys[3], cache_shape, jnp.float32)
    v_cache = (0.8 * value_mean + 0.6 * value_noise).astype(jnp.bfloat16)
    positions = draw_positions(part_keys[4])
    choice_keys = jax.random.split(part_keys[5], 2)
    att_ids = draw_pair(choice_keys[0], ATT_EXPERTS, False)
    mlp_ids = draw_pair(choice_keys[1], MLP_EXPERTS, True)
    norm_att = 1.0 + 0.3 * jax.random.normal(shared_keys[0], (HIDDEN,), jnp.float32)
    w_kv = (jax.random.normal(shared_keys[1], (HIDDEN, KV_HEADS, 2 * HEAD_DIM), jnp.float32) * HIDDEN ** -0.5).astype(jnp.bfloat16)
    router_att = (jax.random.normal(shared_keys[2], (HIDDEN, ATT_EXPERTS), jnp.float32) * 0.5 * HIDDEN ** -0.5).astype(jnp.bfloat16)
    w_query = (jax.random.normal(shared_keys[3], (ATT_EXPERTS, HIDDEN, QUERY_WIDTH), jnp.float32) * HIDDEN ** -0.5).astype(jnp.bfloat16)
    w_out = (jax.random.normal(shared_keys[4], (ATT_EXPERTS, QUERY_WIDTH, HIDDEN), jnp.float32) * QUERY_WIDTH ** -0.5).astype(jnp.bfloat16)
    norm_mlp = 1.0 + 0.3 * jax.random.normal(shared_keys[5], (HIDDEN,), jnp.float32)
    router_mlp = (jax.random.normal(shared_keys[6], (HIDDEN, MLP_EXPERTS), jnp.float32) * 0.5 * HIDDEN ** -0.5).astype(jnp.bfloat16)
    w_gate = (jax.random.normal(shared_keys[7], (MLP_EXPERTS, HIDDEN, FFN_WIDTH), jnp.float32) * HIDDEN ** -0.5).astype(jnp.bfloat16)
    w_up = (jax.random.normal(shared_keys[8], (MLP_EXPERTS, HIDDEN, FFN_WIDTH), jnp.float32) * HIDDEN ** -0.5).astype(jnp.bfloat16)
    w_down = (jax.random.normal(shared_keys[9], (MLP_EXPERTS, FFN_WIDTH, HIDDEN), jnp.float32) * FFN_WIDTH ** -0.5).astype(jnp.bfloat16)
    return {'x': x, 'k_cache': k_cache, 'v_cache': v_cache, 'positions': positions, 'att_ids': att_ids, 'mlp_ids': mlp_ids, 'norm_att': norm_att, 'w_kv': w_kv, 'router_att': router_att, 'w_query': w_query, 'w_out': w_out, 'norm_mlp': norm_mlp, 'router_mlp': router_mlp, 'w_gate': w_gate, 'w_up': w_up, 'w_down': w_down}


def rms_norm(x, gain):
    values = x.astype(jnp.float32)
    inv_rms = lax.rsqrt(jnp.mean(values * values, axis=-1, keepdims=True) + NORM_EPS)
    return (values * inv_rms * gain).astype(jnp.bfloat16)


def rope_tables(positions):
    half_dim = HEAD_DIM // 2
    inv_freq = ROPE_BASE ** (-(jnp.arange(half_dim, dtype=jnp.float32) * 2.0 / HEAD_DIM))
    angles = positions.astype(jnp.float32)[:, None] * inv_freq[None, :]
    return jnp.cos(angles), jnp.sin(angles)


def apply_rope(vectors, cos_table, sin_table):
    half_dim = vectors.shape[-1] // 2
    first_half = vectors[..., :half_dim]
    second_half = vectors[..., half_dim:]
    return jnp.concatenate([first_half * cos_table - second_half * sin_table, second_half * cos_table + first_half * sin_table], axis=-1)


def reference(x, k_cache, v_cache, positions, att_ids, mlp_ids, norm_att, w_kv, router_att, w_query, w_out, norm_mlp, router_mlp, w_gate, w_up, w_down):
    hidden = rms_norm(x, norm_att)
    kv_new = jnp.dot(hidden, w_kv.reshape(HIDDEN, KV_HEADS * 2 * HEAD_DIM), preferred_element_type=jnp.float32).reshape(TOKENS, KV_HEADS, 2 * HEAD_DIM)
    cos_table, sin_table = rope_tables(positions)
    key_new = apply_rope(kv_new[:, :, :HEAD_DIM], cos_table[:, None, :], sin_table[:, None, :]).astype(jnp.bfloat16)
    value_new = kv_new[:, :, HEAD_DIM:].astype(jnp.bfloat16)
    slot_index = jnp.arange(CACHE_LEN)
    at_slot = (slot_index[None, :] == positions[:, None])[:, :, None, None]
    keys_all = jnp.where(at_slot, key_new[:, None, :, :], k_cache)
    values_all = jnp.where(at_slot, value_new[:, None, :, :], v_cache)
    att_logits = jnp.dot(hidden, router_att, preferred_element_type=jnp.float32)
    att_gates = jax.nn.softmax(jnp.take_along_axis(att_logits, att_ids, axis=1), axis=-1)
    query_all = jnp.einsum('bd,edc->bec', hidden.astype(jnp.float32), w_query.astype(jnp.float32))
    query_sel = jnp.take_along_axis(query_all, att_ids[:, :, None], axis=1).reshape(TOKENS, 2, KV_HEADS, HEAD_DIM)
    query_rot = apply_rope(query_sel, cos_table[:, None, None, :], sin_table[:, None, None, :]).astype(jnp.bfloat16)
    scores = jnp.einsum('bknd,bsnd->bkns', query_rot.astype(jnp.float32), keys_all.astype(jnp.float32)) * HEAD_DIM ** -0.5
    visible = (slot_index[None, :] <= positions[:, None])[:, None, None, :]
    weights = jax.nn.softmax(jnp.where(visible, scores, -1e30), axis=-1).astype(jnp.bfloat16)
    attended = jnp.einsum('bkns,bsnd->bknd', weights.astype(jnp.float32), values_all.astype(jnp.float32)).astype(jnp.bfloat16).reshape(TOKENS, 2, QUERY_WIDTH)
    att_onehot = (att_ids[:, :, None] == jnp.arange(ATT_EXPERTS)[None, None, :]).astype(jnp.float32)
    out_slots = jnp.einsum('bke,bkc->bec', att_onehot, attended.astype(jnp.float32))
    projected = jnp.einsum('bec,ecd->bed', out_slots, w_out.astype(jnp.float32))
    att_dense = jnp.einsum('bke,bk->be', att_onehot, att_gates)
    att_sum = jnp.einsum('be,bed->bd', att_dense, projected)
    x_mid = (x.astype(jnp.float32) + att_sum).astype(jnp.bfloat16)
    normed = rms_norm(x_mid, norm_mlp)
    mlp_logits = jnp.dot(normed, router_mlp, preferred_element_type=jnp.float32)
    mlp_gates = jax.nn.softmax(jnp.take_along_axis(mlp_logits, mlp_ids, axis=1), axis=-1)
    mlp_onehot = (mlp_ids[:, :, None] == jnp.arange(MLP_EXPERTS)[None, None, :]).astype(jnp.float32)
    mlp_dense = jnp.einsum('bke,bk->be', mlp_onehot, mlp_gates)

    def expert_step(running_sum, expert_inputs):
        gate_mat, up_mat, down_mat, weight_col = expert_inputs
        gate_val = jnp.dot(normed, gate_mat, preferred_element_type=jnp.float32)
        up_val = jnp.dot(normed, up_mat, preferred_element_type=jnp.float32)
        activation = (jax.nn.silu(gate_val) * up_val).astype(jnp.bfloat16)
        down_out = jnp.dot(activation, down_mat, preferred_element_type=jnp.float32)
        return running_sum + weight_col[:, None] * down_out, None

    mlp_sum, _ = lax.scan(expert_step, jnp.zeros((TOKENS, HIDDEN), jnp.float32), (w_gate, w_up, w_down, mlp_dense.T))
    x_out = (x_mid.astype(jnp.float32) + mlp_sum).astype(jnp.bfloat16)
    return x_out, keys_all, values_all
```

```python
import functools

import jax
import jax.numpy as jnp
import numpy as np
from jax import lax
from jax.experimental import pallas as pl
from jax.experimental.pallas import tpu as pltpu
from jax.sharding import PartitionSpec as P

NORM_EPS = 1e-6
ROPE_BASE = 10000.0
BF = jnp.bfloat16
F32 = jnp.float32
MESH = pl.DeviceIdType.MESH
VMEM_BYTES = 60 * 1024 * 1024

TOK = 512
HID = 2048
HEADS = 4
HD = 128
SLOTS = 16
ATT_E = 8
FFN = 5632
SUB = 64


def vspec():
    return pl.BlockSpec(memory_space=pltpu.VMEM)


def hspec():
    return pl.BlockSpec(memory_space=pl.ANY)


def dot(a, b):
    return jnp.dot(a, b, preferred_element_type=F32)


def dot_nt(a, b):
    return lax.dot_general(a, b, (((1,), (1,)), ((), ())), preferred_element_type=F32)


def norm_rows(x, gain):
    v = x.astype(F32)
    inv = lax.rsqrt(jnp.mean(v * v, axis=-1, keepdims=True) + NORM_EPS)
    return (v * inv * gain).astype(BF)


def columns_of(rows):
    pad = jnp.zeros((128 - rows.shape[0], TOK), F32)
    return jnp.concatenate([rows.astype(F32), pad], axis=0).T


def pair_gates(logits, id0, id1):
    lane = lax.broadcasted_iota(jnp.int32, logits.shape, 1).astype(F32)
    l0 = jnp.sum(jnp.where(lane == id0, logits, 0.0), axis=1, keepdims=True)
    l1 = jnp.sum(jnp.where(lane == id1, logits, 0.0), axis=1, keepdims=True)
    top = jnp.maximum(l0, l1)
    e0 = jnp.exp(l0 - top)
    e1 = jnp.exp(l1 - top)
    total = e0 + e1
    return e0 / total, e1 / total


def attention_kernel(x_ref, gain_ref, wkv_hbm, router_ref, wq_hbm, kc_hbm, vc_hbm, rows_ref, cos_ref, sin_ref,
                     ko_hbm, vo_hbm, o_ref, meta_ref,
                     h, wkv, wq, cosb, sinb, qf, kvb, qb, q8, kn8, vn8, pos8, o8, kin, vin, kout, vout,
                     wkv_sem, wq_sem, kin_sem, vin_sem, ko_sem, vo_sem):
    ring = wq.shape[0]
    steps = TOK // SUB
    cache_rows = SUB * SLOTS * HEADS

    def cache_rows_at(i):
        return pl.ds(pl.multiple_of(i * cache_rows, cache_rows), cache_rows)

    def wq_copy(e):
        return pltpu.make_async_copy(wq_hbm.at[e], wq.at[e % ring], wq_sem.at[e % ring])

    def in_copies(i):
        s = i % 2
        return (pltpu.make_async_copy(kc_hbm.at[cache_rows_at(i)], kin.at[s], kin_sem.at[s]),
                pltpu.make_async_copy(vc_hbm.at[cache_rows_at(i)], vin.at[s], vin_sem.at[s]))

    def out_copies(i):
        s = i % 2
        return (pltpu.make_async_copy(kout.at[s], ko_hbm.at[cache_rows_at(i)], ko_sem.at[s]),
                pltpu.make_async_copy(vout.at[s], vo_hbm.at[cache_rows_at(i)], vo_sem.at[s]))

    wkv_copy = pltpu.make_async_copy(wkv_hbm, wkv, wkv_sem)
    wkv_copy.start()
    for e in range(ring):
        wq_copy(e).start()
    for i in range(2):
        for c in in_copies(i):
            c.start()

    gain = gain_ref[...]

    def norm_step(i, _):
        r = pl.ds(pl.multiple_of(i * 64, 64), 64)
        h[r, :] = norm_rows(x_ref[r, :], gain)
        return 0

    lax.fori_loop(0, TOK // 64, norm_step, 0)

    cols = columns_of(rows_ref[...])
    id0, id1, pos = cols[:, 0:1], cols[:, 1:2], cols[:, 2:3]
    logits = dot_nt(h[...], router_ref[...])
    g0, g1 = pair_gates(logits, id0, id1)
    lane = lax.broadcasted_iota(jnp.int32, (TOK, 128), 1)
    meta_ref[...] = jnp.where(lane == 0, id0, jnp.where(lane == 1, id1, jnp.where(lane == 2, g0, jnp.where(lane == 3, g1, pos))))

    cb = jnp.zeros((TOK, HD), F32)
    sb = jnp.zeros((TOK, HD), F32)
    for p in range(SLOTS):
        hit = pos == float(p)
        cb = jnp.where(hit, cos_ref[p:p + 1, :], cb)
        sb = jnp.where(hit, sin_ref[p:p + 1, :], sb)
    cosb[...] = cb
    sinb[...] = sb

    def rope(v):
        return v * cosb[...] + pltpu.roll(v, HD // 2, 1) * sinb[...]

    wkv_copy.wait()
    half = HEADS * HD
    kf = dot(h[...], wkv[:, 0:half])
    for n in range(HEADS):
        kvb[:, n * HD:(n + 1) * HD] = rope(kf[:, n * HD:(n + 1) * HD]).astype(BF)
    kvb[:, half:2 * half] = dot(h[...], wkv[:, half:2 * half]).astype(BF)

    def query_step(e, _):
        wq_copy(e).wait()
        ef = e.astype(F32)
        qe = dot(h[...], wq[e % ring])
        m0 = meta_ref[:, 0:1] == ef
        m1 = meta_ref[:, 1:2] == ef
        qf[:, 0:half] = jnp.where(m0, qe, qf[:, 0:half])
        qf[:, half:2 * half] = jnp.where(m1, qe, qf[:, half:2 * half])

        @pl.when(e + ring < ATT_E)
        def _():
            wq_copy(e + ring).start()
        return 0

    lax.fori_loop(0, ATT_E, query_step, 0)
    for n in range(2 * HEADS):
        c = slice(n * HD, (n + 1) * HD)
        qb[:, c] = rope(qf[:, c]).astype(BF)

    group = 4
    rows = group * 2 * HEADS
    lane32 = lax.broadcasted_iota(jnp.int32, (rows, 128), 1)
    row32 = lax.broadcasted_iota(jnp.int32, (rows, 128), 0)
    own_part = ((lane32 // 64) == ((row32 // 8) % 2)) & ((lane32 % 4) == (row32 % 4))
    slot32 = ((lane32 // 4) % 16).astype(F32)
    slot_id = (2 * lax.broadcasted_iota(jnp.int32, (8, 8, 128), 0) + lax.broadcasted_iota(jnp.int32, (8, 8, 128), 1) // 4).astype(F32)
    scale = HD ** -0.5
    upper = row32 < rows // 2

    def cache_step(i, _):
        s = i % 2
        r = pl.ds(pl.multiple_of(i * SUB, SUB), SUB)
        for j in range(2 * HEADS):
            q8[pl.ds(j, SUB, stride=8), :] = qb[r, j * HD:(j + 1) * HD].astype(F32)
            n = j % HEADS
            kn8[pl.ds(j, SUB, stride=8), :] = kvb[r, n * HD:(n + 1) * HD].astype(F32)
            vn8[pl.ds(j, SUB, stride=8), :] = kvb[r, half + n * HD:half + (n + 1) * HD].astype(F32)
            pos8[pl.ds(j, SUB, stride=8), :] = jnp.broadcast_to(meta_ref[r, 4:5], (SUB, 128))

        @pl.when(i >= 2)
        def _():
            for c in out_copies(i - 2):
                c.wait()
        for c in in_copies(i):
            c.wait()

        for part in range(SUB // 32):
            scores = []
            for g in range(8):
                b0 = part * 32 + g * group
                rr = slice(b0 * 64, (b0 + group) * 64)
                r8 = slice(b0 * 8, (b0 + group) * 8)
                hit = slot_id[None] == pos8[r8, :].reshape(group, 1, 8, 128)
                old_k = kin[s, rr, :].astype(F32).reshape(group, 8, 8, 128)
                new_k = jnp.where(hit, kn8[r8, :].reshape(group, 1, 8, 128), old_k).astype(BF).reshape(group * 64, 128)
                kout[s, rr, :] = new_k
                old_v = vin[s, rr, :].astype(F32).reshape(group, 8, 8, 128)
                new_v = jnp.where(hit, vn8[r8, :].reshape(group, 1, 8, 128), old_v).astype(BF).reshape(group * 64, 128)
                vout[s, rr, :] = new_v
                sc = dot_nt(q8[r8, :].astype(BF), new_k)
                scores.append(jnp.concatenate([sc[0:rows // 2, 0:128], sc[rows // 2:, 128:256]], axis=0))
            for g in range(8):
                b0 = part * 32 + g * group
                rr = slice(b0 * 64, (b0 + group) * 64)
                r8 = slice(b0 * 8, (b0 + group) * 8)
                valid = own_part & (slot32 <= pos8[r8, :])
                sc = jnp.where(valid, scores[g] * scale, -1e30)
                ex = jnp.exp(sc - jnp.max(sc, axis=1, keepdims=True))
                w = ex / jnp.sum(ex, axis=1, keepdims=True)
                wide = jnp.concatenate([jnp.where(upper, w, 0.0), jnp.where(upper, 0.0, w)], axis=1).astype(BF)
                o8[r8, :] = dot(wide, vout[s, rr, :])

        for c in out_copies(i):
            c.start()

        @pl.when(i + 2 < steps)
        def _():
            for c in in_copies(i + 2):
                c.start()
        for j in range(2 * HEADS):
            o_ref[r, j * HD:(j + 1) * HD] = o8[pl.ds(j, SUB, stride=8), :].astype(BF)
        return 0

    lax.fori_loop(0, steps, cache_step, 0)
    for i in range(steps - 2, steps):
        for c in out_copies(i):
            c.wait()


def attention_call(x, gain, wkv, router_t, wq, kc, vc, rows, cos_tab, sin_tab):
    ring = 4
    cache_rows = SUB * SLOTS * HEADS
    cache = jax.ShapeDtypeStruct(kc.shape, BF)
    return pl.pallas_call(
        attention_kernel,
        out_shape=(cache, cache, jax.ShapeDtypeStruct((TOK, 2 * HEADS * HD), BF), jax.ShapeDtypeStruct((TOK, 128), F32)),
        in_specs=[vspec(), vspec(), hspec(), vspec(), hspec(), hspec(), hspec(), vspec(), vspec(), vspec()],
        out_specs=(hspec(), hspec(), vspec(), vspec()),
        scratch_shapes=[
            pltpu.VMEM((TOK, HID), BF),
            pltpu.VMEM(wkv.shape, BF),
            pltpu.VMEM((ring,) + wq.shape[1:], BF),
            pltpu.VMEM((TOK, HD), F32), pltpu.VMEM((TOK, HD), F32),
            pltpu.VMEM((TOK, 2 * HEADS * HD), F32),
            pltpu.VMEM((TOK, 2 * HEADS * HD), BF),
            pltpu.VMEM((TOK, 2 * HEADS * HD), BF),
            pltpu.VMEM((SUB * 8, 128), F32), pltpu.VMEM((SUB * 8, 128), F32), pltpu.VMEM((SUB * 8, 128), F32),
            pltpu.VMEM((SUB * 8, 128), F32), pltpu.VMEM((SUB * 8, 128), F32),
            pltpu.VMEM((2, cache_rows, HD), BF), pltpu.VMEM((2, cache_rows, HD), BF),
            pltpu.VMEM((2, cache_rows, HD), BF), pltpu.VMEM((2, cache_rows, HD), BF),
            pltpu.SemaphoreType.DMA, pltpu.SemaphoreType.DMA((ring,)),
            pltpu.SemaphoreType.DMA((2,)), pltpu.SemaphoreType.DMA((2,)),
            pltpu.SemaphoreType.DMA((2,)), pltpu.SemaphoreType.DMA((2,)),
        ],
        compiler_params=pltpu.CompilerParams(vmem_limit_bytes=VMEM_BYTES),
        name="attention",
    )(x, gain, wkv, router_t, wq, kc, vc, rows, cos_tab, sin_tab)


HALF = TOK // 2


class PairSum:
    def __init__(self, part, r1, cs, r2, fin, r3, sems):
        self.part, self.r1, self.cs, self.r2, self.fin, self.r3 = part, r1, cs, r2, fin, r3
        self.sems = sems
        me = lax.axis_index("tp")
        chip, core = me // 2, me % 2
        self.sib = chip * 2 + (1 - core)
        self.peer = (1 - chip) * 2 + core
        self.own = pl.ds(pl.multiple_of(core * HALF, HALF), HALF)
        self.other = pl.ds(pl.multiple_of((1 - core) * HALF, HALF), HALF)

    def greet(self):
        barrier = pltpu.get_barrier_semaphore()
        for d in (self.sib, self.peer):
            pl.semaphore_signal(barrier, inc=1, device_id={"tp": d}, device_id_type=MESH)
        pl.semaphore_wait(barrier, 2)

    def copy(self, stage, j):
        src, dst, to = ((self.part.at[j, self.other], self.r1.at[j], self.sib),
                        (self.cs.at[j], self.r2.at[j], self.peer),
                        (self.fin.at[j], self.r3.at[j], self.sib))[stage]
        return pltpu.make_async_remote_copy(src, dst, self.sems.at[0, stage, j], self.sems.at[1, stage, j],
                                            device_id={"tp": to}, device_id_type=MESH)

    def first(self, j):
        self.copy(0, j).start()

    def second(self, j):
        self.copy(0, j).wait()
        self.cs[j] = (self.part[j, self.own].astype(F32) + self.r1[j].astype(F32)).astype(BF)
        self.copy(1, j).start()

    def third(self, j, base_ref, cols):
        self.copy(1, j).wait()
        both = self.cs[j].astype(F32) + self.r2[j].astype(F32)
        self.fin[j] = (base_ref[self.own, cols].astype(F32) + both).astype(BF)
        self.copy(2, j).start()

    def last(self, j, out_ref, cols):
        self.copy(2, j).wait()
        out_ref[self.own, cols] = self.fin[j]
        out_ref[self.other, cols] = self.r3[j]


def pair_scratch(chunks, width):
    return [
        pltpu.VMEM((chunks, TOK, width), BF),
        pltpu.VMEM((chunks, HALF, width), BF), pltpu.VMEM((chunks, HALF, width), BF),
        pltpu.VMEM((chunks, HALF, width), BF), pltpu.VMEM((chunks, HALF, width), BF),
        pltpu.VMEM((chunks, HALF, width), BF),
        pltpu.SemaphoreType.DMA((2, 3, chunks)),
    ]


def project_kernel(x_ref, o_ref, meta_ref, wo_hbm, xm_ref, wo, oe, gb, acc, wo_sem, part, r1, cs, r2, fin, r3, sems):
    chunks, width = part.shape[0], part.shape[2]
    ring = wo.shape[0]
    half = HEADS * HD

    def wo_copy(j):
        return pltpu.make_async_copy(wo_hbm.at[:, :, pl.ds(pl.multiple_of(j * width, width), width)], wo.at[j % ring], wo_sem.at[j % ring])

    for j in range(ring):
        wo_copy(j).start()
    net = PairSum(part, r1, cs, r2, fin, r3, sems)
    net.greet()
    for e in range(ATT_E):
        m0 = meta_ref[:, 0:1] == float(e)
        m1 = meta_ref[:, 1:2] == float(e)
        first = jnp.where(m0, o_ref[:, 0:half].astype(F32), 0.0)
        oe[e] = jnp.where(m1, o_ref[:, half:2 * half].astype(F32), first).astype(BF)
        gate = jnp.where(m0, meta_ref[:, 2:3], jnp.where(m1, meta_ref[:, 3:4], 0.0))
        gb[e] = jnp.broadcast_to(gate, (TOK, 128))

    def chunk_step(j, _):
        wo_copy(j).wait()
        slot = j % ring

        def expert_step(e, _):
            prod = dot(oe[e], wo[slot, e])
            gate = gb[e]
            for n in range(width // 128):
                c = slice(n * 128, (n + 1) * 128)
                acc[:, c] = jnp.where(e == 0, 0.0, acc[:, c]) + gate * prod[:, c]
            return 0

        lax.fori_loop(0, ATT_E, expert_step, 0)
        part[j] = acc[...].astype(BF)

        @pl.when(j + ring < chunks)
        def _():
            wo_copy(j + ring).start()
        net.first(j)
        net.second(j)
        return 0

    lax.fori_loop(0, chunks, chunk_step, 0)
    for j in range(chunks):
        net.third(j, x_ref, slice(j * width, (j + 1) * width))
        if j >= 1:
            net.last(j - 1, xm_ref, slice((j - 1) * width, j * width))
    net.last(chunks - 1, xm_ref, slice((chunks - 1) * width, chunks * width))


def project_call(x, o, meta, wo):
    chunks = 4
    width = HID // chunks
    ring = 2
    return pl.pallas_call(
        project_kernel,
        out_shape=jax.ShapeDtypeStruct((TOK, HID), BF),
        in_specs=[vspec(), vspec(), vspec(), hspec()],
        out_specs=vspec(),
        scratch_shapes=[
            pltpu.VMEM((ring, ATT_E, HEADS * HD, width), BF),
            pltpu.VMEM((ATT_E, TOK, HEADS * HD), BF),
            pltpu.VMEM((ATT_E, TOK, 128), F32),
            pltpu.VMEM((TOK, width), F32),
            pltpu.SemaphoreType.DMA((ring,)),
        ] + pair_scratch(chunks, width),
        compiler_params=pltpu.CompilerParams(vmem_limit_bytes=VMEM_BYTES, collective_id=0, has_side_effects=True),
        name="project_sum",
    )(x, o, meta, wo)


FB = 512
NF = FFN // FB


def gate_up_kernel(xm_ref, gain_ref, router_ref, ids_ref, wg_hbm, wu_hbm, a_hbm, gates_ref,
                   u, pick, spread, xc, wg, wu, ab, count, wg_sem, wu_sem, a_sem):
    ring = wg.shape[0]
    steps = 2 * NF
    first_id = lax.axis_index("tp") * 2

    def in_copies(t):
        f = pl.ds(pl.multiple_of((t % NF) * FB, FB), FB)
        s = t % ring
        return (pltpu.make_async_copy(wg_hbm.at[t // NF, :, f], wg.at[s], wg_sem.at[s]),
                pltpu.make_async_copy(wu_hbm.at[t // NF, :, f], wu.at[s], wu_sem.at[s]))

    def out_copy(t):
        f = pl.ds(pl.multiple_of((t % NF) * FB, FB), FB)
        return pltpu.make_async_copy(ab.at[t % 2], a_hbm.at[t // NF, :, f], a_sem.at[t % 2])

    for t in range(ring):
        for c in in_copies(t):
            c.start()

    gain = gain_ref[...]

    def norm_step(i, _):
        r = pl.ds(pl.multiple_of(i * 64, 64), 64)
        u[r, :] = norm_rows(xm_ref[r, :], gain)
        return 0

    lax.fori_loop(0, TOK // 64, norm_step, 0)
    cols = columns_of(ids_ref[...])
    id0, id1 = cols[:, 0:1], cols[:, 1:2]
    logits = dot_nt(u[...], router_ref[...])
    g0, g1 = pair_gates(logits, id0, id1)
    lane = lax.broadcasted_iota(jnp.int32, (TOK, 128), 1)
    mine = (lane + first_id).astype(F32)
    gates_ref[...] = jnp.where(mine == id0, g0, jnp.where(mine == id1, g1, 0.0))

    def expert_rows(e):
        target = first_id + e
        hit = ((ids_ref[0:1, :] == target) | (ids_ref[1:2, :] == target)).astype(F32)
        before = lax.broadcasted_iota(jnp.int32, (TOK, TOK), 0) < lax.broadcasted_iota(jnp.int32, (TOK, TOK), 1)
        hit8 = jnp.broadcast_to(hit, (8, TOK))
        rank = dot(hit8.astype(BF), before.astype(F32).astype(BF))[0:1, :]
        place = jnp.where(hit > 0.5, rank, -1.0)
        row = lax.broadcasted_iota(jnp.int32, (TOK, TOK), 0).astype(F32)
        sel = (row == place).astype(F32)
        pick[...] = sel.astype(BF)
        spread[...] = sel.T.astype(BF)
        xc[...] = dot(pick[...], u[...]).astype(BF)
        count[0] = (jnp.sum(hit).astype(jnp.int32) + 127) // 128

    def block_step(t, _):
        @pl.when(t % NF == 0)
        def _():
            expert_rows(t // NF)
        s = t % ring
        for c in in_copies(t):
            c.wait()

        @pl.when(t >= 2)
        def _():
            out_copy(t - 2).wait()
        blocks = count[0]

        def run(m):
            g = dot(xc[0:m, :], wg[s])
            up = dot(xc[0:m, :], wu[s])
            act = (jax.nn.silu(g) * up).astype(BF)
            ab[t % 2] = dot(spread[:, 0:m], act).astype(BF)

        for n in range(1, 5):
            @pl.when((blocks == n) if n > 1 else (blocks <= 1))
            def _(n=n):
                run(128 * n)
        out_copy(t).start()

        @pl.when(t + ring < steps)
        def _():
            for c in in_copies(t + ring):
                c.start()
        return 0

    lax.fori_loop(0, steps, block_step, 0)
    for t in range(steps - 2, steps):
        out_copy(t).wait()


def gate_up_call(xm, gain, router_t, ids, wg, wu):
    ring = 4
    return pl.pallas_call(
        gate_up_kernel,
        out_shape=(jax.ShapeDtypeStruct((2, TOK, FFN), BF), jax.ShapeDtypeStruct((TOK, 128), F32)),
        in_specs=[vspec(), vspec(), vspec(), vspec(), hspec(), hspec()],
        out_specs=(hspec(), vspec()),
        scratch_shapes=[
            pltpu.VMEM((TOK, HID), BF), pltpu.VMEM((TOK, TOK), BF), pltpu.VMEM((TOK, TOK), BF), pltpu.VMEM((TOK, HID), BF),
            pltpu.VMEM((ring, HID, FB), BF), pltpu.VMEM((ring, HID, FB), BF), pltpu.VMEM((2, TOK, FB), BF),
            pltpu.SMEM((1,), jnp.int32),
            pltpu.SemaphoreType.DMA((ring,)), pltpu.SemaphoreType.DMA((ring,)), pltpu.SemaphoreType.DMA((2,)),
        ],
        compiler_params=pltpu.CompilerParams(vmem_limit_bytes=VMEM_BYTES),
        name="gate_up",
    )(xm, gain, router_t, ids, wg, wu)


def down_kernel(xm_ref, a_hbm, gates_ref, wd_hbm, out_ref, a, wd, acc, a_sem, wd_sem, part, r1, cs, r2, fin, r3, sems):
    chunks, width = part.shape[0], part.shape[2]
    ring = wd.shape[0]
    total = 2 * chunks

    def wd_copy(t):
        cols = pl.ds(pl.multiple_of((t // 2) * width, width), width)
        return pltpu.make_async_copy(wd_hbm.at[t % 2, :, cols], wd.at[t % ring], wd_sem.at[t % ring])

    for e in range(2):
        pltpu.make_async_copy(a_hbm.at[e], a.at[e], a_sem.at[e]).start()
        wd_copy(e).start()
    for t in range(2, ring):
        wd_copy(t).start()
    net = PairSum(part, r1, cs, r2, fin, r3, sems)
    net.greet()
    for e in range(2):
        pltpu.make_async_copy(a_hbm.at[e], a.at[e], a_sem.at[e]).wait()

    def chunk_step(j, _):
        for e in range(2):
            t = 2 * j + e
            wd_copy(t).wait()
            prod = dot(a[e], wd[t % ring]) * gates_ref[:, e:e + 1]
            if e == 0:
                acc[...] = prod
            else:
                part[j] = (acc[...] + prod).astype(BF)

            @pl.when(t + ring < total)
            def _():
                wd_copy(t + ring).start()
        net.first(j)

        @pl.when(j >= 1)
        def _():
            net.second(j - 1)
        return 0

    lax.fori_loop(0, chunks, chunk_step, 0)
    net.second(chunks - 1)
    for j in range(chunks):
        net.third(j, xm_ref, slice(j * width, (j + 1) * width))
        if j >= 1:
            net.last(j - 1, out_ref, slice((j - 1) * width, j * width))
    net.last(chunks - 1, out_ref, slice((chunks - 1) * width, chunks * width))


def down_call(xm, a, gates, wd):
    chunks = 4
    width = HID // chunks
    ring = 3
    return pl.pallas_call(
        down_kernel,
        out_shape=jax.ShapeDtypeStruct((TOK, HID), BF),
        in_specs=[vspec(), hspec(), vspec(), hspec()],
        out_specs=vspec(),
        scratch_shapes=[
            pltpu.VMEM((2, TOK, FFN), BF),
            pltpu.VMEM((ring, FFN, width), BF),
            pltpu.VMEM((TOK, width), F32),
            pltpu.SemaphoreType.DMA((2,)), pltpu.SemaphoreType.DMA((ring,)),
        ] + pair_scratch(chunks, width),
        compiler_params=pltpu.CompilerParams(vmem_limit_bytes=VMEM_BYTES, collective_id=1, has_side_effects=True),
        name="down_sum",
    )(xm, a, gates, wd)


def rope_tables():
    inv_freq = np.power(np.float64(ROPE_BASE), -(np.arange(HD // 2) * 2.0 / HD))
    angle = (np.arange(SLOTS, dtype=np.float32)[:, None] * inv_freq.astype(np.float32)[None, :]).astype(np.float64)
    cos = np.cos(angle).astype(np.float32)
    sin = np.sin(angle).astype(np.float32)
    return np.concatenate([cos, cos], axis=1), np.concatenate([-sin, sin], axis=1)


def solution(mesh):
    cos_tab, sin_tab = rope_tables()

    def local_step(x, k_cache, v_cache, positions, att_ids, mlp_ids, norm_att, w_kv, router_att, w_query, w_out, norm_mlp, router_mlp, w_gate, w_up, w_down):
        flat = (TOK * SLOTS * HEADS, HD)
        wkv = w_kv.reshape(HID, HEADS, 2, HD).transpose(0, 2, 1, 3).reshape(HID, 2 * HEADS * HD)
        rows = jnp.concatenate([att_ids.T, positions[None, :]], axis=0)
        k_out, v_out, o, meta = attention_call(
            x, norm_att[None, :], wkv, router_att.T, w_query, k_cache.reshape(flat), v_cache.reshape(flat), rows,
            jnp.asarray(cos_tab), jnp.asarray(sin_tab))
        xm = project_call(x, o, meta, w_out)
        a, gates = gate_up_call(xm, norm_mlp[None, :], router_mlp.T, mlp_ids.T, w_gate, w_up)
        x_out = down_call(xm, a, gates, w_down)
        return x_out, k_out.reshape(k_cache.shape), v_out.reshape(v_cache.shape)

    token_spec = P('dp', None)
    cache_spec = P('dp', None, 'tp', None)
    expert_spec = P('tp', None, None)
    in_specs = (token_spec, cache_spec, cache_spec, P('dp'), token_spec, token_spec, P(), P(None, 'tp', None), P(), P(None, None, 'tp'), P(None, 'tp', None), P(), P(), expert_spec, expert_spec, expert_spec)
    out_specs = (token_spec, cache_spec, cache_spec)
    return jax.shard_map(local_step, mesh=mesh, in_specs=in_specs, out_specs=out_specs, check_vma=False)
```

```python
import functools

import jax
import jax.numpy as jnp
import numpy as np
from jax import lax
from jax.experimental import pallas as pl
from jax.experimental.pallas import tpu as pltpu
from jax.sharding import PartitionSpec as P

NORM_EPS = 1e-6
ROPE_BASE = 10000.0
BF = jnp.bfloat16
F32 = jnp.float32
MESH = pl.DeviceIdType.MESH
VMEM_BYTES = 62 * 1024 * 1024

TOK = 512
HID = 2048
HEADS = 4
HD = 128
SLOTS = 16
ATT_E = 8
FFN = 5632
SUB = 64


def vspec():
    return pl.BlockSpec(memory_space=pltpu.VMEM)


def hspec():
    return pl.BlockSpec(memory_space=pl.ANY)


def dot(a, b):
    return jnp.dot(a, b, preferred_element_type=F32)


def dot_nt(a, b):
    return lax.dot_general(a, b, (((1,), (1,)), ((), ())), preferred_element_type=F32)


def norm_rows(x, gain):
    v = x.astype(F32)
    inv = lax.rsqrt(jnp.mean(v * v, axis=-1, keepdims=True) + NORM_EPS)
    return (v * inv * gain).astype(BF)


def columns_of(rows):
    pad = jnp.zeros((128 - rows.shape[0], TOK), F32)
    return jnp.concatenate([rows.astype(F32), pad], axis=0).T


def pair_gates(logits, id0, id1):
    lane = lax.broadcasted_iota(jnp.int32, logits.shape, 1).astype(F32)
    l0 = jnp.sum(jnp.where(lane == id0, logits, 0.0), axis=1, keepdims=True)
    l1 = jnp.sum(jnp.where(lane == id1, logits, 0.0), axis=1, keepdims=True)
    top = jnp.maximum(l0, l1)
    e0 = jnp.exp(l0 - top)
    e1 = jnp.exp(l1 - top)
    total = e0 + e1
    return e0 / total, e1 / total


def attention_kernel(x_ref, gain_ref, wkv_hbm, router_ref, wq_hbm, kc_hbm, vc_hbm, ids_ref, pos_ref, cos_ref, sin_ref,
                     ko_hbm, vo_hbm, o_ref, meta_ref,
                     h, wkv_raw, wkv_wide, wkv, wq, cosb, sinb, qf, kvb, qb, q8, kn8, vn8, pos8, o8, kin, vin, kout, vout,
                     wkv_sem, wq_sem, kin_sem, vin_sem, ko_sem, vo_sem):
    ring = wq.shape[0]
    steps = TOK // SUB
    cache_rows = SUB * SLOTS * HEADS

    def cache_rows_at(i):
        return pl.ds(pl.multiple_of(i * cache_rows, cache_rows), cache_rows)

    def wq_copy(e):
        return pltpu.make_async_copy(wq_hbm.at[e], wq.at[e % ring], wq_sem.at[e % ring])

    def in_copies(i):
        s = i % 2
        return (pltpu.make_async_copy(kc_hbm.at[cache_rows_at(i)], kin.at[s], kin_sem.at[s]),
                pltpu.make_async_copy(vc_hbm.at[cache_rows_at(i)], vin.at[s], vin_sem.at[s]))

    def out_copies(i):
        s = i % 2
        return (pltpu.make_async_copy(kout.at[s], ko_hbm.at[cache_rows_at(i)], ko_sem.at[s]),
                pltpu.make_async_copy(vout.at[s], vo_hbm.at[cache_rows_at(i)], vo_sem.at[s]))

    wkv_copy = pltpu.make_async_copy(wkv_hbm, wkv_raw, wkv_sem)
    wkv_copy.start()
    for e in range(ring):
        wq_copy(e).start()
    for i in range(2):
        for c in in_copies(i):
            c.start()

    gain = gain_ref[...]

    def norm_step(i, _):
        r = pl.ds(pl.multiple_of(i * 64, 64), 64)
        h[r, :] = norm_rows(x_ref[r, :], gain)
        return 0

    lax.fori_loop(0, TOK // 64, norm_step, 0)

    cols = columns_of(jnp.concatenate([ids_ref[...], pos_ref[...]], axis=0))
    id0, id1, pos = cols[:, 0:1], cols[:, 1:2], cols[:, 2:3]
    logits = dot_nt(h[...], router_ref[...])
    g0, g1 = pair_gates(logits, id0, id1)
    lane = lax.broadcasted_iota(jnp.int32, (TOK, 128), 1)
    meta_ref[...] = jnp.where(lane == 0, id0, jnp.where(lane == 1, id1, jnp.where(lane == 2, g0, jnp.where(lane == 3, g1, pos))))

    cb = jnp.zeros((TOK, HD), F32)
    sb = jnp.zeros((TOK, HD), F32)
    for p in range(SLOTS):
        hit = pos == float(p)
        cb = jnp.where(hit, cos_ref[p:p + 1, :], cb)
        sb = jnp.where(hit, sin_ref[p:p + 1, :], sb)
    cosb[...] = cb
    sinb[...] = sb

    def rope(v):
        return v * cosb[...] + pltpu.roll(v, HD // 2, 1) * sinb[...]

    wkv_copy.wait()
    half = HEADS * HD
    deep = wkv_wide.shape[0] // 8

    def relayout_step(i, _):
        wkv_wide[...] = wkv_raw[pl.ds(pl.multiple_of(i * deep * 8, deep * 8), deep * 8), :].astype(F32)
        for j in range(8):
            wkv[pl.ds(pl.multiple_of(i * deep, deep), deep), j * HD:(j + 1) * HD] = wkv_wide[pl.ds(j, deep, stride=8), :].astype(BF)
        return 0

    lax.fori_loop(0, HID // deep, relayout_step, 0)
    kf = dot(h[...], wkv[:, 0:half])
    for n in range(HEADS):
        kvb[:, n * HD:(n + 1) * HD] = rope(kf[:, n * HD:(n + 1) * HD]).astype(BF)
    kvb[:, half:2 * half] = dot(h[...], wkv[:, half:2 * half]).astype(BF)

    def query_step(e, _):
        wq_copy(e).wait()
        ef = e.astype(F32)
        qe = dot(h[...], wq[e % ring])
        m0 = meta_ref[:, 0:1] == ef
        m1 = meta_ref[:, 1:2] == ef
        qf[:, 0:half] = jnp.where(m0, qe, qf[:, 0:half])
        qf[:, half:2 * half] = jnp.where(m1, qe, qf[:, half:2 * half])

        @pl.when(e + ring < ATT_E)
        def _():
            wq_copy(e + ring).start()
        return 0

    lax.fori_loop(0, ATT_E, query_step, 0)
    for n in range(2 * HEADS):
        c = slice(n * HD, (n + 1) * HD)
        qb[:, c] = rope(qf[:, c]).astype(BF)

    group = 4
    rows = group * 2 * HEADS
    lane32 = lax.broadcasted_iota(jnp.int32, (rows, 128), 1)
    row32 = lax.broadcasted_iota(jnp.int32, (rows, 128), 0)
    own_part = ((lane32 // 64) == ((row32 // 8) % 2)) & ((lane32 % 4) == (row32 % 4))
    slot32 = ((lane32 // 4) % 16).astype(F32)
    slot_id = (2 * lax.broadcasted_iota(jnp.int32, (8, 8, 128), 0) + lax.broadcasted_iota(jnp.int32, (8, 8, 128), 1) // 4).astype(F32)
    scale = HD ** -0.5
    upper = row32 < rows // 2

    def cache_step(i, _):
        s = i % 2
        r = pl.ds(pl.multiple_of(i * SUB, SUB), SUB)
        for j in range(2 * HEADS):
            q8[pl.ds(j, SUB, stride=8), :] = qb[r, j * HD:(j + 1) * HD].astype(F32)
            n = j % HEADS
            kn8[pl.ds(j, SUB, stride=8), :] = kvb[r, n * HD:(n + 1) * HD].astype(F32)
            vn8[pl.ds(j, SUB, stride=8), :] = kvb[r, half + n * HD:half + (n + 1) * HD].astype(F32)
            pos8[pl.ds(j, SUB, stride=8), :] = jnp.broadcast_to(meta_ref[r, 4:5], (SUB, 128))

        @pl.when(i >= 2)
        def _():
            for c in out_copies(i - 2):
                c.wait()
        for c in in_copies(i):
            c.wait()

        for part in range(SUB // 32):
            scores = []
            for g in range(8):
                b0 = part * 32 + g * group
                rr = slice(b0 * 64, (b0 + group) * 64)
                r8 = slice(b0 * 8, (b0 + group) * 8)
                hit = slot_id[None] == pos8[r8, :].reshape(group, 1, 8, 128)
                old_k = kin[s, rr, :].astype(F32).reshape(group, 8, 8, 128)
                new_k = jnp.where(hit, kn8[r8, :].reshape(group, 1, 8, 128), old_k).astype(BF).reshape(group * 64, 128)
                kout[s, rr, :] = new_k
                old_v = vin[s, rr, :].astype(F32).reshape(group, 8, 8, 128)
                new_v = jnp.where(hit, vn8[r8, :].reshape(group, 1, 8, 128), old_v).astype(BF).reshape(group * 64, 128)
                vout[s, rr, :] = new_v
                sc = dot_nt(q8[r8, :].astype(BF), new_k)
                scores.append(jnp.concatenate([sc[0:rows // 2, 0:128], sc[rows // 2:, 128:256]], axis=0))
            for g in range(8):
                b0 = part * 32 + g * group
                rr = slice(b0 * 64, (b0 + group) * 64)
                r8 = slice(b0 * 8, (b0 + group) * 8)
                valid = own_part & (slot32 <= pos8[r8, :])
                sc = jnp.where(valid, scores[g] * scale, -1e30)
                ex = jnp.exp(sc - jnp.max(sc, axis=1, keepdims=True))
                w = ex / jnp.sum(ex, axis=1, keepdims=True)
                wide = jnp.concatenate([jnp.where(upper, w, 0.0), jnp.where(upper, 0.0, w)], axis=1).astype(BF)
                o8[r8, :] = dot(wide, vout[s, rr, :])

        for c in out_copies(i):
            c.start()

        @pl.when(i + 2 < steps)
        def _():
            for c in in_copies(i + 2):
                c.start()
        for j in range(2 * HEADS):
            o_ref[r, j * HD:(j + 1) * HD] = o8[pl.ds(j, SUB, stride=8), :].astype(BF)
        return 0

    lax.fori_loop(0, steps, cache_step, 0)
    for i in range(steps - 2, steps):
        for c in out_copies(i):
            c.wait()


def attention_call(x, gain, wkv, router_t, wq, kc, vc, ids, pos, cos_tab, sin_tab):
    ring = 4
    cache_rows = SUB * SLOTS * HEADS
    cache = jax.ShapeDtypeStruct(kc.shape, BF)
    return pl.pallas_call(
        attention_kernel,
        out_shape=(cache, cache, jax.ShapeDtypeStruct((TOK, 2 * HEADS * HD), BF), jax.ShapeDtypeStruct((TOK, 128), F32)),
        in_specs=[vspec(), vspec(), hspec(), vspec(), hspec(), hspec(), hspec(), vspec(), vspec(), vspec(), vspec()],
        out_specs=(hspec(), hspec(), vspec(), vspec()),
        scratch_shapes=[
            pltpu.VMEM((TOK, HID), BF),
            pltpu.VMEM(wkv.shape, BF), pltpu.VMEM((2048, HD), F32), pltpu.VMEM((HID, 2 * HEADS * HD), BF),
            pltpu.VMEM((ring,) + wq.shape[1:], BF),
            pltpu.VMEM((TOK, HD), F32), pltpu.VMEM((TOK, HD), F32),
            pltpu.VMEM((TOK, 2 * HEADS * HD), F32),
            pltpu.VMEM((TOK, 2 * HEADS * HD), BF),
            pltpu.VMEM((TOK, 2 * HEADS * HD), BF),
            pltpu.VMEM((SUB * 8, 128), F32), pltpu.VMEM((SUB * 8, 128), F32), pltpu.VMEM((SUB * 8, 128), F32),
            pltpu.VMEM((SUB * 8, 128), F32), pltpu.VMEM((SUB * 8, 128), F32),
            pltpu.VMEM((2, cache_rows, HD), BF), pltpu.VMEM((2, cache_rows, HD), BF),
            pltpu.VMEM((2, cache_rows, HD), BF), pltpu.VMEM((2, cache_rows, HD), BF),
            pltpu.SemaphoreType.DMA, pltpu.SemaphoreType.DMA((ring,)),
            pltpu.SemaphoreType.DMA((2,)), pltpu.SemaphoreType.DMA((2,)),
            pltpu.SemaphoreType.DMA((2,)), pltpu.SemaphoreType.DMA((2,)),
        ],
        compiler_params=pltpu.CompilerParams(vmem_limit_bytes=VMEM_BYTES),
        name="attention",
    )(x, gain, wkv, router_t, wq, kc, vc, ids, pos, cos_tab, sin_tab)


HALF = TOK // 2


class PairSum:
    def __init__(self, part_at, r1, cs, r2, fin, r3, sems):
        self.part_at, self.r1, self.cs, self.r2, self.fin, self.r3 = part_at, r1, cs, r2, fin, r3
        self.sems = sems
        self.width = r1.shape[2]
        me = lax.axis_index("tp")
        chip, core = me // 2, me % 2
        self.sib = chip * 2 + (1 - core)
        self.peer = (1 - chip) * 2 + core
        self.own = pl.ds(pl.multiple_of(core * HALF, HALF), HALF)
        self.other = pl.ds(pl.multiple_of((1 - core) * HALF, HALF), HALF)

    def greet(self):
        barrier = pltpu.get_barrier_semaphore()
        for d in (self.sib, self.peer):
            pl.semaphore_signal(barrier, inc=1, device_id={"tp": d}, device_id_type=MESH)
        pl.semaphore_wait(barrier, 2)

    def cols(self, j):
        return pl.ds(pl.multiple_of(j * self.width, self.width), self.width)

    def copy(self, stage, j):
        src, dst, to = ((self.part_at(j, self.other), self.r1.at[j], self.sib),
                        (self.cs.at[j], self.r2.at[j], self.peer),
                        (self.fin.at[j], self.r3.at[j], self.sib))[stage]
        return pltpu.make_async_remote_copy(src, dst, self.sems.at[0, stage, j], self.sems.at[1, stage, j],
                                            device_id={"tp": to}, device_id_type=MESH)

    def first(self, j):
        self.copy(0, j).start()

    def second(self, j):
        self.copy(0, j).wait()
        self.cs[j] = (self.part_at(j, self.own)[...].astype(F32) + self.r1[j].astype(F32)).astype(BF)
        self.copy(1, j).start()

    def third(self, j, base_ref):
        self.copy(1, j).wait()
        both = self.cs[j].astype(F32) + self.r2[j].astype(F32)
        self.fin[j] = (base_ref[self.own, self.cols(j)].astype(F32) + both).astype(BF)
        self.copy(2, j).start()

    def last(self, j, out_ref):
        self.copy(2, j).wait()
        out_ref[self.own, self.cols(j)] = self.fin[j]
        out_ref[self.other, self.cols(j)] = self.r3[j]

    def finish(self, chunks, base_ref, out_ref):
        def step(j, _):
            self.third(j, base_ref)

            @pl.when(j >= 1)
            def _():
                self.last(j - 1, out_ref)
            return 0

        lax.fori_loop(0, chunks, step, 0)
        self.last(chunks - 1, out_ref)


def pair_scratch(chunks, width):
    return [pltpu.VMEM((chunks, HALF, width), BF)] * 5 + [pltpu.SemaphoreType.DMA((2, 3, chunks))]


def project_kernel(x_hbm, o_ref, meta_ref, wo_hbm, xm_ref, xv, wo, oe, gb, acc, x_sem, wo_sem, part, r1, cs, r2, fin, r3, sems):
    chunks, width = part.shape[0], part.shape[2]
    ring = wo.shape[0]
    half = HEADS * HD

    def wo_copy(j):
        return pltpu.make_async_copy(wo_hbm.at[:, :, pl.ds(pl.multiple_of(j * width, width), width)], wo.at[j % ring], wo_sem.at[j % ring])

    for j in range(ring):
        wo_copy(j).start()
    x_copy = pltpu.make_async_copy(x_hbm, xv, x_sem)
    x_copy.start()
    net = PairSum(lambda j, rows: part.at[j, rows], r1, cs, r2, fin, r3, sems)
    net.greet()
    for e in range(ATT_E):
        m0 = meta_ref[:, 0:1] == float(e)
        m1 = meta_ref[:, 1:2] == float(e)
        f0 = jnp.broadcast_to(jnp.where(m0, 1.0, 0.0), (TOK, 128)).astype(BF)
        f1 = jnp.broadcast_to(jnp.where(m1, 1.0, 0.0), (TOK, 128)).astype(BF)
        for n in range(HEADS):
            c = slice(n * HD, (n + 1) * HD)
            oe[e, :, c] = o_ref[:, c] * f0 + o_ref[:, half + n * HD:half + (n + 1) * HD] * f1
        gate = jnp.where(m0, meta_ref[:, 2:3], jnp.where(m1, meta_ref[:, 3:4], 0.0))
        gb[e] = jnp.broadcast_to(gate, (TOK, 128))

    def chunk_step(j, _):
        wo_copy(j).wait()
        slot = j % ring

        def expert_step(e, _):
            prod = dot(oe[e], wo[slot, e])
            gate = gb[e]
            for n in range(width // 128):
                c = slice(n * 128, (n + 1) * 128)
                acc[:, c] = jnp.where(e == 0, 0.0, acc[:, c]) + gate * prod[:, c]
            return 0

        lax.fori_loop(0, ATT_E, expert_step, 0)
        part[j] = acc[...].astype(BF)

        @pl.when(j + ring < chunks)
        def _():
            wo_copy(j + ring).start()
        net.first(j)

        @pl.when(j == 0)
        def _():
            net.second(j)

        @pl.when(j >= 2)
        def _():
            net.second(j - 1)
        return 0

    lax.fori_loop(0, chunks, chunk_step, 0)
    net.second(chunks - 1)
    x_copy.wait()
    net.finish(chunks, xv, xm_ref)


def project_call(x, o, meta, wo):
    chunks = 8
    width = HID // chunks
    ring = 3
    return pl.pallas_call(
        project_kernel,
        out_shape=jax.ShapeDtypeStruct((TOK, HID), BF),
        in_specs=[hspec(), vspec(), vspec(), hspec()],
        out_specs=vspec(),
        scratch_shapes=[
            pltpu.VMEM((TOK, HID), BF),
            pltpu.VMEM((ring, ATT_E, HEADS * HD, width), BF),
            pltpu.VMEM((ATT_E, TOK, HEADS * HD), BF),
            pltpu.VMEM((ATT_E, TOK, 128), F32),
            pltpu.VMEM((TOK, width), F32),
            pltpu.SemaphoreType.DMA, pltpu.SemaphoreType.DMA((ring,)),
            pltpu.VMEM((chunks, TOK, width), BF),
        ] + pair_scratch(chunks, width),
        compiler_params=pltpu.CompilerParams(vmem_limit_bytes=VMEM_BYTES, collective_id=0, has_side_effects=True),
        name="project_sum",
    )(x, o, meta, wo)


FB = 512
NF = FFN // FB
DB = 512
ND = HID // DB


def experts_kernel(xm_ref, gain_ref, router_ref, ids_ref, wg_hbm, wu_hbm, wd_hbm, y_ref,
                   u, pick, spread, xc, ac, gc, wg, wu, wd, count, wg_sem, wu_sem, wd_sem):
    ring = wg.shape[0]
    dring = wd.shape[0]
    steps = 2 * NF
    dsteps = 2 * ND
    first_id = lax.axis_index("tp") * 2

    def in_copies(t):
        f = pl.ds(pl.multiple_of((t % NF) * FB, FB), FB)
        s = t % ring
        return (pltpu.make_async_copy(wg_hbm.at[t // NF, :, f], wg.at[s], wg_sem.at[s]),
                pltpu.make_async_copy(wu_hbm.at[t // NF, :, f], wu.at[s], wu_sem.at[s]))

    def down_copy(t):
        c = pl.ds(pl.multiple_of((t // 2) * DB, DB), DB)
        return pltpu.make_async_copy(wd_hbm.at[t % 2, :, c], wd.at[t % dring], wd_sem.at[t % dring])

    for t in range(ring):
        for c in in_copies(t):
            c.start()

    gain = gain_ref[...]

    def norm_step(i, _):
        r = pl.ds(pl.multiple_of(i * 64, 64), 64)
        u[r, :] = norm_rows(xm_ref[r, :], gain)
        return 0

    lax.fori_loop(0, TOK // 64, norm_step, 0)
    cols = columns_of(ids_ref[...])
    id0, id1 = cols[:, 0:1], cols[:, 1:2]
    logits = dot_nt(u[...], router_ref[...])
    g0, g1 = pair_gates(logits, id0, id1)
    lane = lax.broadcasted_iota(jnp.int32, (TOK, 128), 1)
    mine = (lane + first_id).astype(F32)
    gates = jnp.where(mine == id0, g0, jnp.where(mine == id1, g1, 0.0)).T

    row = lax.broadcasted_iota(jnp.int32, (TOK, TOK), 0)
    before = (row < lax.broadcasted_iota(jnp.int32, (TOK, TOK), 1)).astype(F32).astype(BF)
    for e in range(2):
        target = first_id + e
        hit = ((ids_ref[0:1, :] == target) | (ids_ref[1:2, :] == target)).astype(F32)
        rank = dot(jnp.broadcast_to(hit, (8, TOK)).astype(BF), before)[0:1, :]
        place = jnp.where(hit > 0.5, rank, -1.0)
        sel = (row.astype(F32) == place).astype(F32)
        pick[...] = sel.astype(BF)
        spread[e] = sel.T.astype(BF)
        gc[e] = jnp.broadcast_to(jnp.sum(sel * gates[e:e + 1, :], axis=1, keepdims=True), (TOK, 128))
        xc[e] = dot(pick[...], u[...]).astype(BF)
        count[e] = (jnp.sum(hit).astype(jnp.int32) + 127) // 128

    def by_blocks(blocks, run):
        for n in range(1, 5):
            @pl.when((blocks == n) if n > 1 else (blocks <= 1))
            def _(n=n):
                run(128 * n)

    def block_step(t, _):
        e = t // NF
        s = t % ring
        f = pl.ds(pl.multiple_of((t % NF) * FB, FB), FB)
        for c in in_copies(t):
            c.wait()

        def run(m):
            g = dot(xc[e, 0:m, :], wg[s])
            up = dot(xc[e, 0:m, :], wu[s])
            ac[e, 0:m, f] = (jax.nn.silu(g) * up).astype(BF)

        by_blocks(count[e], run)

        @pl.when(t + ring < steps)
        def _():
            for c in in_copies(t + ring):
                c.start()

        @pl.when((t + ring >= steps) & (t + ring < steps + dring))
        def _():
            down_copy(t + ring - steps).start()
        return 0

    lax.fori_loop(0, steps, block_step, 0)

    def down_step(t, _):
        e = t % 2
        s = t % dring
        c = pl.ds(pl.multiple_of((t // 2) * DB, DB), DB)
        down_copy(t).wait()

        def run(m):
            d = dot(ac[e, 0:m, :], wd[s])
            gate = gc[e, 0:m, :]
            parts = [(d[:, n * 128:(n + 1) * 128] * gate).astype(BF) for n in range(DB // 128)]
            back = dot(spread[e, :, 0:m], jnp.concatenate(parts, axis=1))
            y_ref[:, c] = (jnp.where(e == 0, 0.0, y_ref[:, c].astype(F32)) + back).astype(BF)

        by_blocks(count[e], run)

        @pl.when(t + dring < dsteps)
        def _():
            down_copy(t + dring).start()
        return 0

    lax.fori_loop(0, dsteps, down_step, 0)


def experts_call(xm, gain, router_t, ids, wg, wu, wd):
    ring = 4
    dring = 3
    return pl.pallas_call(
        experts_kernel,
        out_shape=jax.ShapeDtypeStruct((TOK, HID), BF),
        in_specs=[vspec(), vspec(), vspec(), vspec(), hspec(), hspec(), hspec()],
        out_specs=vspec(),
        scratch_shapes=[
            pltpu.VMEM((TOK, HID), BF), pltpu.VMEM((TOK, TOK), BF), pltpu.VMEM((2, TOK, TOK), BF), pltpu.VMEM((2, TOK, HID), BF),
            pltpu.VMEM((2, TOK, FFN), BF), pltpu.VMEM((2, TOK, 128), F32),
            pltpu.VMEM((ring, HID, FB), BF), pltpu.VMEM((ring, HID, FB), BF), pltpu.VMEM((dring, FFN, DB), BF),
            pltpu.SMEM((2,), jnp.int32),
            pltpu.SemaphoreType.DMA((ring,)), pltpu.SemaphoreType.DMA((ring,)), pltpu.SemaphoreType.DMA((dring,)),
        ],
        compiler_params=pltpu.CompilerParams(vmem_limit_bytes=VMEM_BYTES),
        name="experts",
    )(xm, gain, router_t, ids, wg, wu, wd)


def sum_kernel(xm_ref, y_ref, out_ref, r1, cs, r2, fin, r3, sems):
    chunks, width = r1.shape[0], r1.shape[2]
    net = PairSum(lambda j, rows: y_ref.at[rows, pl.ds(pl.multiple_of(j * width, width), width)], r1, cs, r2, fin, r3, sems)
    net.greet()
    for j in range(chunks):
        net.first(j)

    def step(j, _):
        net.second(j)
        return 0

    lax.fori_loop(0, chunks, step, 0)
    net.finish(chunks, xm_ref, out_ref)


def sum_call(xm, y):
    chunks = 8
    width = HID // chunks
    return pl.pallas_call(
        sum_kernel,
        out_shape=jax.ShapeDtypeStruct((TOK, HID), BF),
        in_specs=[vspec(), vspec()],
        out_specs=vspec(),
        scratch_shapes=pair_scratch(chunks, width),
        compiler_params=pltpu.CompilerParams(vmem_limit_bytes=32 * 1024 * 1024, collective_id=1, has_side_effects=True),
        name="expert_sum",
    )(xm, y)


def rope_tables():
    inv_freq = np.power(np.float64(ROPE_BASE), -(np.arange(HD // 2) * 2.0 / HD))
    angle = (np.arange(SLOTS, dtype=np.float32)[:, None] * inv_freq.astype(np.float32)[None, :]).astype(np.float64)
    cos = np.cos(angle).astype(np.float32)
    sin = np.sin(angle).astype(np.float32)
    return np.concatenate([cos, cos], axis=1), np.concatenate([-sin, sin], axis=1)


def solution(mesh):
    cos_tab, sin_tab = rope_tables()

    def local_step(x, k_cache, v_cache, positions, att_ids, mlp_ids, norm_att, w_kv, router_att, w_query, w_out, norm_mlp, router_mlp, w_gate, w_up, w_down):
        flat = (TOK * SLOTS * HEADS, HD)
        wkv = w_kv.reshape(HID, HEADS, 2, HD).transpose(0, 2, 1, 3).reshape(HID * 2 * HEADS, HD)
        k_out, v_out, o, meta = attention_call(
            x, norm_att[None, :], wkv, router_att.T, w_query, k_cache.reshape(flat), v_cache.reshape(flat), att_ids.T, positions[None, :],
            jnp.asarray(cos_tab), jnp.asarray(sin_tab))
        xm = project_call(x, o, meta, w_out)
        y = experts_call(xm, norm_mlp[None, :], router_mlp.T, mlp_ids.T, w_gate, w_up, w_down)
        x_out = sum_call(xm, y)
        return x_out, k_out.reshape(k_cache.shape), v_out.reshape(v_cache.shape)

    token_spec = P('dp', None)
    cache_spec = P('dp', None, 'tp', None)
    expert_spec = P('tp', None, None)
    in_specs = (token_spec, cache_spec, cache_spec, P('dp'), token_spec, token_spec, P(), P(None, 'tp', None), P(), P(None, None, 'tp'), P(None, 'tp', None), P(), P(), expert_spec, expert_spec, expert_spec)
    out_specs = (token_spec, cache_spec, cache_spec)
    return jax.shard_map(local_step, mesh=mesh, in_specs=in_specs, out_specs=out_specs, check_vma=False)
```

```python
import functools

import jax
import jax.numpy as jnp
import numpy as np
from jax import lax
from jax.experimental import pallas as pl
from jax.experimental.pallas import tpu as pltpu
from jax.sharding import PartitionSpec as P

NORM_EPS = 1e-6
ROPE_BASE = 10000.0
BF = jnp.bfloat16
F32 = jnp.float32
MESH = pl.DeviceIdType.MESH
VMEM_BYTES = 62 * 1024 * 1024

TOK = 512
HID = 2048
HEADS = 4
HD = 128
SLOTS = 16
ATT_E = 8
FFN = 5632
SUB = 64


def vspec():
    return pl.BlockSpec(memory_space=pltpu.VMEM)


def hspec():
    return pl.BlockSpec(memory_space=pl.ANY)


def dot(a, b):
    return jnp.dot(a, b, preferred_element_type=F32)


def dot_nt(a, b):
    return lax.dot_general(a, b, (((1,), (1,)), ((), ())), preferred_element_type=F32)


def norm_rows(x, gain):
    v = x.astype(F32)
    inv = lax.rsqrt(jnp.mean(v * v, axis=-1, keepdims=True) + NORM_EPS)
    return (v * inv * gain).astype(BF)


def columns_of(rows):
    pad = jnp.zeros((128 - rows.shape[0], TOK), F32)
    return jnp.concatenate([rows.astype(F32), pad], axis=0).T


def pair_gates(logits, id0, id1):
    lane = lax.broadcasted_iota(jnp.int32, logits.shape, 1).astype(F32)
    l0 = jnp.sum(jnp.where(lane == id0, logits, 0.0), axis=1, keepdims=True)
    l1 = jnp.sum(jnp.where(lane == id1, logits, 0.0), axis=1, keepdims=True)
    top = jnp.maximum(l0, l1)
    e0 = jnp.exp(l0 - top)
    e1 = jnp.exp(l1 - top)
    total = e0 + e1
    return e0 / total, e1 / total


def attention_kernel(x_ref, gain_ref, wkv_hbm, router_ref, wq_hbm, kc_hbm, vc_hbm, ids_ref, pos_ref, cos_ref, sin_ref,
                     ko_hbm, vo_hbm, o_ref, meta_ref,
                     h, wkv_raw, wkv_wide, wkv, wq, cosb, sinb, qf, kvb, qb, q8, kn8, vn8, pos8, o8, kin, vin, kout, vout,
                     wkv_sem, wq_sem, kin_sem, vin_sem, ko_sem, vo_sem):
    ring = wq.shape[0]
    steps = TOK // SUB
    depth = kin.shape[0]
    back = kout.shape[0]
    cache_rows = SUB * SLOTS * HEADS

    def cache_rows_at(i):
        return pl.ds(pl.multiple_of(i * cache_rows, cache_rows), cache_rows)

    def wq_copy(e):
        return pltpu.make_async_copy(wq_hbm.at[e], wq.at[e % ring], wq_sem.at[e % ring])

    def in_copies(i):
        s = i % depth
        return (pltpu.make_async_copy(kc_hbm.at[cache_rows_at(i)], kin.at[s], kin_sem.at[s]),
                pltpu.make_async_copy(vc_hbm.at[cache_rows_at(i)], vin.at[s], vin_sem.at[s]))

    def out_copies(i):
        s = i % back
        return (pltpu.make_async_copy(kout.at[s], ko_hbm.at[cache_rows_at(i)], ko_sem.at[s]),
                pltpu.make_async_copy(vout.at[s], vo_hbm.at[cache_rows_at(i)], vo_sem.at[s]))

    wkv_copy = pltpu.make_async_copy(wkv_hbm, wkv_raw, wkv_sem)
    wq_copy(0).start()
    wkv_copy.start()
    for e in range(1, ring):
        wq_copy(e).start()
    for i in range(depth):
        for c in in_copies(i):
            c.start()

    gain = gain_ref[...]

    def norm_step(i, _):
        r = pl.ds(pl.multiple_of(i * 64, 64), 64)
        h[r, :] = norm_rows(x_ref[r, :], gain)
        return 0

    lax.fori_loop(0, TOK // 64, norm_step, 0)

    cols = columns_of(jnp.concatenate([ids_ref[...], pos_ref[...]], axis=0))
    id0, id1, pos = cols[:, 0:1], cols[:, 1:2], cols[:, 2:3]
    logits = dot_nt(h[...], router_ref[...])
    g0, g1 = pair_gates(logits, id0, id1)
    lane = lax.broadcasted_iota(jnp.int32, (TOK, 128), 1)
    meta_ref[...] = jnp.where(lane == 0, id0, jnp.where(lane == 1, id1, jnp.where(lane == 2, g0, jnp.where(lane == 3, g1, pos))))

    cb = jnp.zeros((TOK, HD), F32)
    sb = jnp.zeros((TOK, HD), F32)
    for p in range(SLOTS):
        hit = pos == float(p)
        cb = jnp.where(hit, cos_ref[p:p + 1, :], cb)
        sb = jnp.where(hit, sin_ref[p:p + 1, :], sb)
    cosb[...] = cb
    sinb[...] = sb

    def rope(v):
        return v * cosb[...] + pltpu.roll(v, HD // 2, 1) * sinb[...]

    wkv_copy.wait()
    half = HEADS * HD
    deep = HID // ATT_E

    def query_step(e, _):
        wq_copy(e).wait()
        ef = e.astype(F32)
        qe = dot(h[...], wq[e % ring])
        m0 = meta_ref[:, 0:1] == ef
        m1 = meta_ref[:, 1:2] == ef
        qf[:, 0:half] = jnp.where(m0, qe, qf[:, 0:half])
        qf[:, half:2 * half] = jnp.where(m1, qe, qf[:, half:2 * half])
        wkv_wide[...] = wkv_raw[pl.ds(pl.multiple_of(e * deep * 8, deep * 8), deep * 8), :].astype(F32)
        for j in range(8):
            wkv[pl.ds(pl.multiple_of(e * deep, deep), deep), j * HD:(j + 1) * HD] = wkv_wide[pl.ds(j, deep, stride=8), :].astype(BF)

        @pl.when(e + ring < ATT_E)
        def _():
            wq_copy(e + ring).start()
        return 0

    lax.fori_loop(0, ATT_E, query_step, 0)
    kf = dot(h[...], wkv[:, 0:half])
    for n in range(HEADS):
        kvb[:, n * HD:(n + 1) * HD] = rope(kf[:, n * HD:(n + 1) * HD]).astype(BF)
    kvb[:, half:2 * half] = dot(h[...], wkv[:, half:2 * half]).astype(BF)
    for n in range(2 * HEADS):
        c = slice(n * HD, (n + 1) * HD)
        qb[:, c] = rope(qf[:, c]).astype(BF)

    group = 4
    rows = group * 2 * HEADS
    lane32 = lax.broadcasted_iota(jnp.int32, (rows, 128), 1)
    row32 = lax.broadcasted_iota(jnp.int32, (rows, 128), 0)
    own_part = ((lane32 // 64) == ((row32 // 8) % 2)) & ((lane32 % 4) == (row32 % 4))
    slot32 = ((lane32 // 4) % 16).astype(F32)
    slot_id = (2 * lax.broadcasted_iota(jnp.int32, (8, 8, 128), 0) + lax.broadcasted_iota(jnp.int32, (8, 8, 128), 1) // 4).astype(F32)
    scale = HD ** -0.5
    upper = row32 < rows // 2

    def cache_step(i, _):
        s = i % depth
        so = i % back
        r = pl.ds(pl.multiple_of(i * SUB, SUB), SUB)
        for j in range(2 * HEADS):
            q8[pl.ds(j, SUB, stride=8), :] = qb[r, j * HD:(j + 1) * HD].astype(F32)
            n = j % HEADS
            kn8[pl.ds(j, SUB, stride=8), :] = kvb[r, n * HD:(n + 1) * HD].astype(F32)
            vn8[pl.ds(j, SUB, stride=8), :] = kvb[r, half + n * HD:half + (n + 1) * HD].astype(F32)
            pos8[pl.ds(j, SUB, stride=8), :] = jnp.broadcast_to(meta_ref[r, 4:5], (SUB, 128))

        @pl.when(i >= back)
        def _():
            for c in out_copies(i - back):
                c.wait()
        for c in in_copies(i):
            c.wait()

        def group_rows(g):
            return slice(g * group * 64, (g + 1) * group * 64), slice(g * group * 8, (g + 1) * group * 8)

        for part in range(SUB // 32):
            groups = range(part * 8, part * 8 + 8, 2)
            scores = []
            for g0 in groups:
                keys, queries = [], []
                for g in (g0, g0 + 1):
                    rr, r8 = group_rows(g)
                    hit = slot_id[None] == pos8[r8, :].reshape(group, 1, 8, 128)
                    old_k = kin[s, rr, :].astype(F32).reshape(group, 8, 8, 128)
                    new_k = jnp.where(hit, kn8[r8, :].reshape(group, 1, 8, 128), old_k).reshape(group * 64, 128).astype(BF)
                    kout[so, rr, :] = new_k
                    old_v = vin[s, rr, :].astype(F32).reshape(group, 8, 8, 128)
                    new_v = jnp.where(hit, vn8[r8, :].reshape(group, 1, 8, 128), old_v).reshape(group * 64, 128).astype(BF)
                    vout[so, rr, :] = new_v
                    keys.append(new_k)
                    queries.append(q8[r8, :].astype(BF))
                none = jnp.zeros((rows, 128), BF)
                both = jnp.concatenate([jnp.concatenate([queries[0], none], axis=1), jnp.concatenate([none, queries[1]], axis=1)], axis=0)
                sc = dot_nt(both, jnp.concatenate(keys, axis=1))
                for b in (0, rows):
                    scores.append(jnp.concatenate([sc[b:b + rows // 2, 0:128], sc[b + rows // 2:b + rows, 128:256]], axis=0))
            for n, g0 in enumerate(groups):
                wides, values = [], []
                for b in range(2):
                    rr, r8 = group_rows(g0 + b)
                    valid = own_part & (slot32 <= pos8[r8, :])
                    sc = jnp.where(valid, scores[2 * n + b] * scale, -1e30)
                    ex = jnp.exp(sc - jnp.max(sc, axis=1, keepdims=True))
                    w = ex / jnp.sum(ex, axis=1, keepdims=True)
                    wides.append(jnp.concatenate([jnp.where(upper, w, 0.0), jnp.where(upper, 0.0, w)], axis=1).astype(BF))
                    values.append(vout[so, rr, :])
                res = dot(jnp.concatenate(wides, axis=0), jnp.concatenate(values, axis=1))
                for b in range(2):
                    o8[group_rows(g0 + b)[1], :] = res[b * rows:(b + 1) * rows, b * 128:(b + 1) * 128]

        for c in out_copies(i):
            c.start()

        @pl.when(i + depth < steps)
        def _():
            for c in in_copies(i + depth):
                c.start()
        for j in range(2 * HEADS):
            o_ref[r, j * HD:(j + 1) * HD] = o8[pl.ds(j, SUB, stride=8), :].astype(BF)
        return 0

    lax.fori_loop(0, steps, cache_step, 0)
    for i in range(steps - back, steps):
        for c in out_copies(i):
            c.wait()


def attention_call(x, gain, wkv, router_t, wq, kc, vc, ids, pos, cos_tab, sin_tab):
    ring = 4
    depth = 2
    back = 2
    cache_rows = SUB * SLOTS * HEADS
    cache = jax.ShapeDtypeStruct(kc.shape, BF)
    return pl.pallas_call(
        attention_kernel,
        out_shape=(cache, cache, jax.ShapeDtypeStruct((TOK, 2 * HEADS * HD), BF), jax.ShapeDtypeStruct((TOK, 128), F32)),
        in_specs=[vspec(), vspec(), hspec(), vspec(), hspec(), hspec(), hspec(), vspec(), vspec(), vspec(), vspec()],
        out_specs=(hspec(), hspec(), vspec(), vspec()),
        scratch_shapes=[
            pltpu.VMEM((TOK, HID), BF),
            pltpu.VMEM(wkv.shape, BF), pltpu.VMEM((2048, HD), F32), pltpu.VMEM((HID, 2 * HEADS * HD), BF),
            pltpu.VMEM((ring,) + wq.shape[1:], BF),
            pltpu.VMEM((TOK, HD), F32), pltpu.VMEM((TOK, HD), F32),
            pltpu.VMEM((TOK, 2 * HEADS * HD), F32),
            pltpu.VMEM((TOK, 2 * HEADS * HD), BF),
            pltpu.VMEM((TOK, 2 * HEADS * HD), BF),
            pltpu.VMEM((SUB * 8, 128), F32), pltpu.VMEM((SUB * 8, 128), F32), pltpu.VMEM((SUB * 8, 128), F32),
            pltpu.VMEM((SUB * 8, 128), F32), pltpu.VMEM((SUB * 8, 128), F32),
            pltpu.VMEM((depth, cache_rows, HD), BF), pltpu.VMEM((depth, cache_rows, HD), BF),
            pltpu.VMEM((back, cache_rows, HD), BF), pltpu.VMEM((back, cache_rows, HD), BF),
            pltpu.SemaphoreType.DMA, pltpu.SemaphoreType.DMA((ring,)),
            pltpu.SemaphoreType.DMA((depth,)), pltpu.SemaphoreType.DMA((depth,)),
            pltpu.SemaphoreType.DMA((back,)), pltpu.SemaphoreType.DMA((back,)),
        ],
        compiler_params=pltpu.CompilerParams(vmem_limit_bytes=VMEM_BYTES),
        name="attention",
    )(x, gain, wkv, router_t, wq, kc, vc, ids, pos, cos_tab, sin_tab)


HALF = TOK // 2


class PairSum:
    def __init__(self, part_at, r1, cs, r2, fin, r3, sems):
        self.part_at, self.r1, self.cs, self.r2, self.fin, self.r3 = part_at, r1, cs, r2, fin, r3
        self.own_at = lambda j: part_at(j, self.own)
        self.sems = sems
        self.width = r1.shape[2]
        me = lax.axis_index("tp")
        chip, core = me // 2, me % 2
        self.sib = chip * 2 + (1 - core)
        self.peer = (1 - chip) * 2 + core
        self.own = pl.ds(pl.multiple_of(core * HALF, HALF), HALF)
        self.other = pl.ds(pl.multiple_of((1 - core) * HALF, HALF), HALF)

    def greet(self):
        barrier = pltpu.get_barrier_semaphore()
        for d in (self.sib, self.peer):
            pl.semaphore_signal(barrier, inc=1, device_id={"tp": d}, device_id_type=MESH)
        pl.semaphore_wait(barrier, 2)

    def cols(self, j):
        return pl.ds(pl.multiple_of(j * self.width, self.width), self.width)

    def copy(self, stage, j):
        src, dst, to = ((self.part_at(j, self.other), self.r1.at[j], self.sib),
                        (self.cs.at[j], self.r2.at[j], self.peer),
                        (self.fin.at[j], self.r3.at[j], self.sib))[stage]
        return pltpu.make_async_remote_copy(src, dst, self.sems.at[0, stage, j], self.sems.at[1, stage, j],
                                            device_id={"tp": to}, device_id_type=MESH)

    def first(self, j):
        self.copy(0, j).start()

    def second(self, j):
        self.copy(0, j).wait()
        self.cs[j] = (self.own_at(j)[...].astype(F32) + self.r1[j].astype(F32)).astype(BF)
        self.copy(1, j).start()

    def third(self, j, base_ref):
        self.copy(1, j).wait()
        both = self.cs[j].astype(F32) + self.r2[j].astype(F32)
        self.fin[j] = (base_ref[self.own, self.cols(j)].astype(F32) + both).astype(BF)
        self.copy(2, j).start()

    def last(self, j, out_ref):
        self.copy(2, j).wait()
        out_ref[self.own, self.cols(j)] = self.fin[j]
        out_ref[self.other, self.cols(j)] = self.r3[j]

    def finish(self, chunks, base_ref, out_ref):
        def step(j, _):
            self.third(j, base_ref)

            @pl.when(j >= 1)
            def _():
                self.last(j - 1, out_ref)
            return 0

        lax.fori_loop(0, chunks, step, 0)
        self.last(chunks - 1, out_ref)


def pair_scratch(chunks, width):
    return [pltpu.VMEM((chunks, HALF, width), BF)] * 5 + [pltpu.SemaphoreType.DMA((2, 3, chunks))]


def project_kernel(x_hbm, o_ref, meta_ref, wo_hbm, xm_ref, xv, wo, oe, gb, acc, x_sem, wo_sem, part, r1, cs, r2, fin, r3, sems):
    chunks, width = part.shape[0], part.shape[2]
    ring = wo.shape[0]
    half = HEADS * HD

    def wo_copy(j):
        return pltpu.make_async_copy(wo_hbm.at[:, :, pl.ds(pl.multiple_of(j * width, width), width)], wo.at[j % ring], wo_sem.at[j % ring])

    for j in range(ring):
        wo_copy(j).start()
    x_copy = pltpu.make_async_copy(x_hbm, xv, x_sem)
    x_copy.start()
    net = PairSum(lambda j, rows: part.at[j, rows], r1, cs, r2, fin, r3, sems)
    net.greet()

    def prepare(e):
        m0 = meta_ref[:, 0:1] == float(e)
        m1 = meta_ref[:, 1:2] == float(e)
        f0 = jnp.broadcast_to(jnp.where(m0, 1.0, 0.0), (TOK, 128)).astype(BF)
        f1 = jnp.broadcast_to(jnp.where(m1, 1.0, 0.0), (TOK, 128)).astype(BF)
        for n in range(HEADS):
            c = slice(n * HD, (n + 1) * HD)
            oe[e, :, c] = o_ref[:, c] * f0 + o_ref[:, half + n * HD:half + (n + 1) * HD] * f1
        gate = jnp.where(m0, meta_ref[:, 2:3], jnp.where(m1, meta_ref[:, 3:4], 0.0))
        gb[e] = jnp.broadcast_to(gate, (TOK, 128))

    def project(j, fresh):
        wo_copy(j).wait()
        slot = j % ring
        for e in range(ATT_E):
            if fresh:
                prepare(e)
            prod = dot(oe[e], wo[slot, e])
            for n in range(width // 128):
                c = slice(n * 128, (n + 1) * 128)
                term = gb[e] * prod[:, c]
                if e == 0:
                    acc[:, c] = term
                elif e < ATT_E - 1:
                    acc[:, c] += term
                else:
                    part[j, :, c] = (acc[:, c] + term).astype(BF)
        net.first(j)

    def chunk_step(j, _):
        project(j, False)

        @pl.when(j + ring < chunks)
        def _():
            wo_copy(j + ring).start()

        @pl.when(j >= 2)
        def _():
            net.second(j - 1)
        return 0

    project(0, True)
    wo_copy(ring).start()
    net.second(0)
    lax.fori_loop(1, chunks, chunk_step, 0)
    net.second(chunks - 1)
    x_copy.wait()
    net.finish(chunks, xv, xm_ref)


def project_call(x, o, meta, wo):
    chunks = 8
    width = HID // chunks
    ring = 3
    return pl.pallas_call(
        project_kernel,
        out_shape=jax.ShapeDtypeStruct((TOK, HID), BF),
        in_specs=[hspec(), vspec(), vspec(), hspec()],
        out_specs=vspec(),
        scratch_shapes=[
            pltpu.VMEM((TOK, HID), BF),
            pltpu.VMEM((ring, ATT_E, HEADS * HD, width), BF),
            pltpu.VMEM((ATT_E, TOK, HEADS * HD), BF),
            pltpu.VMEM((ATT_E, TOK, 128), F32),
            pltpu.VMEM((TOK, width), F32),
            pltpu.SemaphoreType.DMA, pltpu.SemaphoreType.DMA((ring,)),
            pltpu.VMEM((chunks, TOK, width), BF),
        ] + pair_scratch(chunks, width),
        compiler_params=pltpu.CompilerParams(vmem_limit_bytes=VMEM_BYTES, collective_id=0, has_side_effects=True),
        name="project_sum",
    )(x, o, meta, wo)


FB = 512
NF = FFN // FB
DB = 512
ND = HID // DB
ROW_STEPS = (128, 192, 256, 320, 384, 512)


def experts_kernel(xm_ref, gain_ref, router_ref, ids_ref, wg_hbm, wu_hbm, wd_hbm, y_ref,
                   u, pick, spread, xc, ac, gc, wg, wu, wd, count, wg_sem, wu_sem, wd_sem):
    ring = wg.shape[0]
    dring = wd.shape[0]
    steps = 2 * NF
    dsteps = 2 * ND
    first_id = lax.axis_index("tp") * 2

    def in_copies(t):
        f = pl.ds(pl.multiple_of((t // 2) * FB, FB), FB)
        s = t % ring
        return (pltpu.make_async_copy(wg_hbm.at[t % 2, :, f], wg.at[s], wg_sem.at[s]),
                pltpu.make_async_copy(wu_hbm.at[t % 2, :, f], wu.at[s], wu_sem.at[s]))

    def down_copy(t):
        c = pl.ds(pl.multiple_of((t // 2) * DB, DB), DB)
        return pltpu.make_async_copy(wd_hbm.at[t % 2, :, c], wd.at[t % dring], wd_sem.at[t % dring])

    for t in range(ring):
        for c in in_copies(t):
            c.start()

    gain = gain_ref[...]

    def norm_step(i, _):
        r = pl.ds(pl.multiple_of(i * 64, 64), 64)
        u[r, :] = norm_rows(xm_ref[r, :], gain)
        return 0

    lax.fori_loop(0, TOK // 64, norm_step, 0)
    cols = columns_of(ids_ref[...])
    id0, id1 = cols[:, 0:1], cols[:, 1:2]
    logits = dot_nt(u[...], router_ref[...])
    g0, g1 = pair_gates(logits, id0, id1)
    lane = lax.broadcasted_iota(jnp.int32, (TOK, 128), 1)
    mine = (lane + first_id).astype(F32)
    gates = jnp.where(mine == id0, g0, jnp.where(mine == id1, g1, 0.0)).T

    row = lax.broadcasted_iota(jnp.int32, (TOK, TOK), 0)
    before = (row < lax.broadcasted_iota(jnp.int32, (TOK, TOK), 1)).astype(F32).astype(BF)
    for e in range(2):
        target = first_id + e
        hit = ((ids_ref[0:1, :] == target) | (ids_ref[1:2, :] == target)).astype(F32)
        rank = dot(jnp.broadcast_to(hit, (8, TOK)).astype(BF), before)[0:1, :]
        place = jnp.where(hit > 0.5, rank, -1.0)
        sel = (row.astype(F32) == place).astype(F32)
        pick[...] = sel.astype(BF)
        spread[e] = sel.T.astype(BF)
        gc[e] = jnp.broadcast_to(jnp.sum(sel * gates[e:e + 1, :], axis=1, keepdims=True), (TOK, 128))
        xc[e] = dot(pick[...], u[...]).astype(BF)
        count[e] = (jnp.sum(hit).astype(jnp.int32) + 63) // 64

    def by_blocks(blocks, run):
        for low, high in zip((0,) + ROW_STEPS[:-1], ROW_STEPS):
            @pl.when((blocks * 64 > low) & (blocks * 64 <= high) if low else blocks * 64 <= high)
            def _(high=high):
                run(high)

    def block_step(t, _):
        e = t % 2
        s = t % ring
        f = pl.ds(pl.multiple_of((t // 2) * FB, FB), FB)
        for c in in_copies(t):
            c.wait()

        def run(m):
            g = dot(xc[e, 0:m, :], wg[s])
            up = dot(xc[e, 0:m, :], wu[s])
            ac[e, 0:m, f] = (jax.nn.silu(g) * up).astype(BF)

        by_blocks(count[e], run)

        @pl.when(t + ring < steps)
        def _():
            for c in in_copies(t + ring):
                c.start()

        @pl.when((t + ring >= steps) & (t + ring < steps + dring))
        def _():
            down_copy(t + ring - steps).start()
        return 0

    lax.fori_loop(0, steps, block_step, 0)

    def down_step(t, _):
        e = t % 2
        s = t % dring
        c = pl.ds(pl.multiple_of((t // 2) * DB, DB), DB)
        down_copy(t).wait()

        def run(m):
            d = dot(ac[e, 0:m, :], wd[s])
            gate = gc[e, 0:m, :]
            parts = [(d[:, n * 128:(n + 1) * 128] * gate).astype(BF) for n in range(DB // 128)]
            back = dot(spread[e, :, 0:m], jnp.concatenate(parts, axis=1))
            y_ref[:, c] = (jnp.where(e == 0, 0.0, y_ref[:, c].astype(F32)) + back).astype(BF)

        by_blocks(count[e], run)

        @pl.when(t + dring < dsteps)
        def _():
            down_copy(t + dring).start()
        return 0

    lax.fori_loop(0, dsteps, down_step, 0)


def experts_call(xm, gain, router_t, ids, wg, wu, wd):
    ring = 4
    dring = 3
    return pl.pallas_call(
        experts_kernel,
        out_shape=jax.ShapeDtypeStruct((TOK, HID), BF),
        in_specs=[vspec(), vspec(), vspec(), vspec(), hspec(), hspec(), hspec()],
        out_specs=vspec(),
        scratch_shapes=[
            pltpu.VMEM((TOK, HID), BF), pltpu.VMEM((TOK, TOK), BF), pltpu.VMEM((2, TOK, TOK), BF), pltpu.VMEM((2, TOK, HID), BF),
            pltpu.VMEM((2, TOK, FFN), BF), pltpu.VMEM((2, TOK, 128), F32),
            pltpu.VMEM((ring, HID, FB), BF), pltpu.VMEM((ring, HID, FB), BF), pltpu.VMEM((dring, FFN, DB), BF),
            pltpu.SMEM((2,), jnp.int32),
            pltpu.SemaphoreType.DMA((ring,)), pltpu.SemaphoreType.DMA((ring,)), pltpu.SemaphoreType.DMA((dring,)),
        ],
        compiler_params=pltpu.CompilerParams(vmem_limit_bytes=VMEM_BYTES),
        name="experts",
    )(xm, gain, router_t, ids, wg, wu, wd)


def sum_kernel(xm_hbm, y_hbm, out_ref, xv, yv, in_sem, r1, cs, r2, fin, r3, sems):
    chunks, width = r1.shape[0], r1.shape[2]

    def y_at(j, rows):
        return y_hbm.at[rows, pl.ds(pl.multiple_of(j * width, width), width)]

    net = PairSum(y_at, r1, cs, r2, fin, r3, sems)
    x_copy = pltpu.make_async_copy(xm_hbm.at[net.own], xv.at[net.own], in_sem.at[0])
    y_copy = pltpu.make_async_copy(y_hbm.at[net.own], yv.at[net.own], in_sem.at[1])
    y_copy.start()
    x_copy.start()
    net.greet()
    for j in range(chunks):
        net.first(j)
    y_copy.wait()
    net.own_at = lambda j: yv.at[net.own, net.cols(j)]

    def step(j, _):
        net.second(j)
        return 0

    lax.fori_loop(0, chunks, step, 0)
    x_copy.wait()
    net.finish(chunks, xv, out_ref)


def sum_call(xm, y):
    chunks = 8
    width = HID // chunks
    return pl.pallas_call(
        sum_kernel,
        out_shape=jax.ShapeDtypeStruct((TOK, HID), BF),
        in_specs=[hspec(), hspec()],
        out_specs=vspec(),
        scratch_shapes=[pltpu.VMEM((TOK, HID), BF), pltpu.VMEM((TOK, HID), BF), pltpu.SemaphoreType.DMA((2,))] + pair_scratch(chunks, width),
        compiler_params=pltpu.CompilerParams(vmem_limit_bytes=61 * 1024 * 1024, collective_id=1, has_side_effects=True),
        name="expert_sum",
    )(xm, y)


def rope_tables():
    inv_freq = np.power(np.float64(ROPE_BASE), -(np.arange(HD // 2) * 2.0 / HD))
    angle = (np.arange(SLOTS, dtype=np.float32)[:, None] * inv_freq.astype(np.float32)[None, :]).astype(np.float64)
    cos = np.cos(angle).astype(np.float32)
    sin = np.sin(angle).astype(np.float32)
    return np.concatenate([cos, cos], axis=1), np.concatenate([-sin, sin], axis=1)


def solution(mesh):
    cos_tab, sin_tab = rope_tables()

    def local_step(x, k_cache, v_cache, positions, att_ids, mlp_ids, norm_att, w_kv, router_att, w_query, w_out, norm_mlp, router_mlp, w_gate, w_up, w_down):
        flat = (TOK * SLOTS * HEADS, HD)
        wkv = w_kv.reshape(HID, HEADS, 2, HD).transpose(0, 2, 1, 3).reshape(HID * 2 * HEADS, HD)
        k_out, v_out, o, meta = attention_call(
            x, norm_att[None, :], wkv, router_att.T, w_query, k_cache.reshape(flat), v_cache.reshape(flat), att_ids.T, positions[None, :],
            jnp.asarray(cos_tab), jnp.asarray(sin_tab))
        xm = project_call(x, o, meta, w_out)
        y = experts_call(xm, norm_mlp[None, :], router_mlp.T, mlp_ids.T, w_gate, w_up, w_down)
        x_out = sum_call(xm, y)
        return x_out, k_out.reshape(k_cache.shape), v_out.reshape(v_cache.shape)

    token_spec = P('dp', None)
    cache_spec = P('dp', None, 'tp', None)
    expert_spec = P('tp', None, None)
    in_specs = (token_spec, cache_spec, cache_spec, P('dp'), token_spec, token_spec, P(), P(None, 'tp', None), P(), P(None, None, 'tp'), P(None, 'tp', None), P(), P(), expert_spec, expert_spec, expert_spec)
    out_specs = (token_spec, cache_spec, cache_spec)
    return jax.shard_map(local_step, mesh=mesh, in_specs=in_specs, out_specs=out_specs, check_vma=False)
```

```python
import functools

import jax
import jax.numpy as jnp
import numpy as np
from jax import lax
from jax.experimental import pallas as pl
from jax.experimental.pallas import tpu as pltpu
from jax.sharding import PartitionSpec as P

NORM_EPS = 1e-6
ROPE_BASE = 10000.0
BF = jnp.bfloat16
F32 = jnp.float32
MESH = pl.DeviceIdType.MESH
VMEM_BYTES = 62 * 1024 * 1024

TOK = 512
HID = 2048
HEADS = 4
HD = 128
SLOTS = 16
ATT_E = 8
FFN = 5632
SUB = 64


def vspec():
    return pl.BlockSpec(memory_space=pltpu.VMEM)


def hspec():
    return pl.BlockSpec(memory_space=pl.ANY)


def dot(a, b):
    return jnp.dot(a, b, preferred_element_type=F32)


def dot_nt(a, b):
    return lax.dot_general(a, b, (((1,), (1,)), ((), ())), preferred_element_type=F32)


def norm_rows(x, gain):
    v = x.astype(F32)
    inv = lax.rsqrt(jnp.mean(v * v, axis=-1, keepdims=True) + NORM_EPS)
    return (v * inv * gain).astype(BF)


def columns_of(rows):
    pad = jnp.zeros((128 - rows.shape[0], TOK), F32)
    return jnp.concatenate([rows.astype(F32), pad], axis=0).T


def pair_gates(logits, id0, id1):
    lane = lax.broadcasted_iota(jnp.int32, logits.shape, 1).astype(F32)
    l0 = jnp.sum(jnp.where(lane == id0, logits, 0.0), axis=1, keepdims=True)
    l1 = jnp.sum(jnp.where(lane == id1, logits, 0.0), axis=1, keepdims=True)
    top = jnp.maximum(l0, l1)
    e0 = jnp.exp(l0 - top)
    e1 = jnp.exp(l1 - top)
    total = e0 + e1
    return e0 / total, e1 / total


def attention_kernel(x_ref, gain_ref, wkv_hbm, router_ref, wq_hbm, kc_hbm, vc_hbm, ids_ref, pos_ref, cos_ref, sin_ref,
                     ko_hbm, vo_hbm, o_ref, meta_ref,
                     h, wkv_raw, wkv_wide, wkv, wq, cosb, sinb, qf, kvb, qb, q8, kn8, vn8, pos8, o8, kin, vin, kout, vout,
                     wkv_sem, wq_sem, kin_sem, vin_sem, ko_sem, vo_sem):
    ring = wq.shape[0]
    steps = TOK // SUB
    depth = kin.shape[0]
    back = kout.shape[0]
    cache_rows = SUB * SLOTS * HEADS

    def cache_rows_at(i):
        return pl.ds(pl.multiple_of(i * cache_rows, cache_rows), cache_rows)

    def wq_copy(e):
        return pltpu.make_async_copy(wq_hbm.at[e], wq.at[e % ring], wq_sem.at[e % ring])

    def in_copies(i):
        s = i % depth
        return (pltpu.make_async_copy(kc_hbm.at[cache_rows_at(i)], kin.at[s], kin_sem.at[s]),
                pltpu.make_async_copy(vc_hbm.at[cache_rows_at(i)], vin.at[s], vin_sem.at[s]))

    def out_copies(i):
        s = i % back
        return (pltpu.make_async_copy(kout.at[s], ko_hbm.at[cache_rows_at(i)], ko_sem.at[s]),
                pltpu.make_async_copy(vout.at[s], vo_hbm.at[cache_rows_at(i)], vo_sem.at[s]))

    wkv_copy = pltpu.make_async_copy(wkv_hbm, wkv_raw, wkv_sem)
    wq_copy(0).start()
    wkv_copy.start()
    for e in range(1, ring):
        wq_copy(e).start()

    gain = gain_ref[...]

    def norm_step(i, _):
        r = pl.ds(pl.multiple_of(i * 64, 64), 64)
        h[r, :] = norm_rows(x_ref[r, :], gain)
        return 0

    lax.fori_loop(0, TOK // 64, norm_step, 0)

    cols = columns_of(jnp.concatenate([ids_ref[...], pos_ref[...]], axis=0))
    id0, id1, pos = cols[:, 0:1], cols[:, 1:2], cols[:, 2:3]
    logits = dot_nt(h[...], router_ref[...])
    g0, g1 = pair_gates(logits, id0, id1)
    lane = lax.broadcasted_iota(jnp.int32, (TOK, 128), 1)
    meta_ref[...] = jnp.where(lane == 0, id0, jnp.where(lane == 1, id1, jnp.where(lane == 2, g0, jnp.where(lane == 3, g1, pos))))

    cb = jnp.zeros((TOK, HD), F32)
    sb = jnp.zeros((TOK, HD), F32)
    for p in range(SLOTS):
        hit = pos == float(p)
        cb = jnp.where(hit, cos_ref[p:p + 1, :], cb)
        sb = jnp.where(hit, sin_ref[p:p + 1, :], sb)
    cosb[...] = cb
    sinb[...] = sb

    def rope(v):
        return v * cosb[...] + pltpu.roll(v, HD // 2, 1) * sinb[...]

    wkv_copy.wait()
    half = HEADS * HD
    deep = HID // ATT_E

    def query_step(e, _):
        wq_copy(e).wait()

        @pl.when(e < depth)
        def _():
            for c in in_copies(e):
                c.start()
        ef = e.astype(F32)
        qe = dot(h[...], wq[e % ring])
        m0 = meta_ref[:, 0:1] == ef
        m1 = meta_ref[:, 1:2] == ef
        qf[:, 0:half] = jnp.where(m0, qe, qf[:, 0:half])
        qf[:, half:2 * half] = jnp.where(m1, qe, qf[:, half:2 * half])
        wkv_wide[...] = wkv_raw[pl.ds(pl.multiple_of(e * deep * 8, deep * 8), deep * 8), :].astype(F32)
        for j in range(8):
            wkv[pl.ds(pl.multiple_of(e * deep, deep), deep), j * HD:(j + 1) * HD] = wkv_wide[pl.ds(j, deep, stride=8), :].astype(BF)

        @pl.when(e + ring < ATT_E)
        def _():
            wq_copy(e + ring).start()
        return 0

    lax.fori_loop(0, ATT_E, query_step, 0)
    kf = dot(h[...], wkv[:, 0:half])
    for n in range(HEADS):
        kvb[:, n * HD:(n + 1) * HD] = rope(kf[:, n * HD:(n + 1) * HD]).astype(BF)
    kvb[:, half:2 * half] = dot(h[...], wkv[:, half:2 * half]).astype(BF)
    for n in range(2 * HEADS):
        c = slice(n * HD, (n + 1) * HD)
        qb[:, c] = rope(qf[:, c]).astype(BF)

    group = 4
    rows = group * 2 * HEADS
    lane32 = lax.broadcasted_iota(jnp.int32, (rows, 128), 1)
    row32 = lax.broadcasted_iota(jnp.int32, (rows, 128), 0)
    own_part = ((lane32 // 64) == ((row32 // 8) % 2)) & ((lane32 % 4) == (row32 % 4))
    slot32 = ((lane32 // 4) % 16).astype(F32)
    slot_id = (2 * lax.broadcasted_iota(jnp.int32, (8, 8, 128), 0) + lax.broadcasted_iota(jnp.int32, (8, 8, 128), 1) // 4).astype(F32)
    scale = HD ** -0.5
    upper = row32 < rows // 2

    def cache_step(i, _):
        s = i % depth
        so = i % back
        r = pl.ds(pl.multiple_of(i * SUB, SUB), SUB)
        for j in range(2 * HEADS):
            q8[pl.ds(j, SUB, stride=8), :] = qb[r, j * HD:(j + 1) * HD].astype(F32)
            n = j % HEADS
            kn8[pl.ds(j, SUB, stride=8), :] = kvb[r, n * HD:(n + 1) * HD].astype(F32)
            vn8[pl.ds(j, SUB, stride=8), :] = kvb[r, half + n * HD:half + (n + 1) * HD].astype(F32)
            pos8[pl.ds(j, SUB, stride=8), :] = jnp.broadcast_to(meta_ref[r, 4:5], (SUB, 128))

        @pl.when(i >= back)
        def _():
            for c in out_copies(i - back):
                c.wait()
        for c in in_copies(i):
            c.wait()

        def group_rows(g):
            return slice(g * group * 64, (g + 1) * group * 64), slice(g * group * 8, (g + 1) * group * 8)

        for part in range(SUB // 32):
            groups = range(part * 8, part * 8 + 8, 2)
            scores = []
            for g0 in groups:
                keys, queries = [], []
                for g in (g0, g0 + 1):
                    rr, r8 = group_rows(g)
                    hit = slot_id[None] == pos8[r8, :].reshape(group, 1, 8, 128)
                    old_k = kin[s, rr, :].astype(F32).reshape(group, 8, 8, 128)
                    new_k = jnp.where(hit, kn8[r8, :].reshape(group, 1, 8, 128), old_k).reshape(group * 64, 128).astype(BF)
                    kout[so, rr, :] = new_k
                    old_v = vin[s, rr, :].astype(F32).reshape(group, 8, 8, 128)
                    new_v = jnp.where(hit, vn8[r8, :].reshape(group, 1, 8, 128), old_v).reshape(group * 64, 128).astype(BF)
                    vout[so, rr, :] = new_v
                    keys.append(new_k)
                    queries.append(q8[r8, :].astype(BF))
                none = jnp.zeros((rows, 128), BF)
                both = jnp.concatenate([jnp.concatenate([queries[0], none], axis=1), jnp.concatenate([none, queries[1]], axis=1)], axis=0)
                sc = dot_nt(both, jnp.concatenate(keys, axis=1))
                for b in (0, rows):
                    scores.append(jnp.concatenate([sc[b:b + rows // 2, 0:128], sc[b + rows // 2:b + rows, 128:256]], axis=0))
            for n, g0 in enumerate(groups):
                wides, values = [], []
                for b in range(2):
                    rr, r8 = group_rows(g0 + b)
                    valid = own_part & (slot32 <= pos8[r8, :])
                    sc = jnp.where(valid, scores[2 * n + b] * scale, -1e30)
                    ex = jnp.exp(sc - jnp.max(sc, axis=1, keepdims=True))
                    w = ex / jnp.sum(ex, axis=1, keepdims=True)
                    wides.append(jnp.concatenate([jnp.where(upper, w, 0.0), jnp.where(upper, 0.0, w)], axis=1).astype(BF))
                    values.append(vout[so, rr, :])
                res = dot(jnp.concatenate(wides, axis=0), jnp.concatenate(values, axis=1))
                for b in range(2):
                    o8[group_rows(g0 + b)[1], :] = res[b * rows:(b + 1) * rows, b * 128:(b + 1) * 128]

        for c in out_copies(i):
            c.start()

        @pl.when(i + depth < steps)
        def _():
            for c in in_copies(i + depth):
                c.start()
        for j in range(2 * HEADS):
            o_ref[r, j * HD:(j + 1) * HD] = o8[pl.ds(j, SUB, stride=8), :].astype(BF)
        return 0

    lax.fori_loop(0, steps, cache_step, 0)
    for i in range(steps - back, steps):
        for c in out_copies(i):
            c.wait()


def attention_call(x, gain, wkv, router_t, wq, kc, vc, ids, pos, cos_tab, sin_tab):
    ring = 4
    depth = 4
    back = 2
    cache_rows = SUB * SLOTS * HEADS
    cache = jax.ShapeDtypeStruct(kc.shape, BF)
    return pl.pallas_call(
        attention_kernel,
        out_shape=(cache, cache, jax.ShapeDtypeStruct((TOK, 2 * HEADS * HD), BF), jax.ShapeDtypeStruct((TOK, 128), F32)),
        in_specs=[vspec(), vspec(), hspec(), vspec(), hspec(), hspec(), hspec(), vspec(), vspec(), vspec(), vspec()],
        out_specs=(hspec(), hspec(), vspec(), vspec()),
        scratch_shapes=[
            pltpu.VMEM((TOK, HID), BF),
            pltpu.VMEM(wkv.shape, BF), pltpu.VMEM((2048, HD), F32), pltpu.VMEM((HID, 2 * HEADS * HD), BF),
            pltpu.VMEM((ring,) + wq.shape[1:], BF),
            pltpu.VMEM((TOK, HD), F32), pltpu.VMEM((TOK, HD), F32),
            pltpu.VMEM((TOK, 2 * HEADS * HD), F32),
            pltpu.VMEM((TOK, 2 * HEADS * HD), BF),
            pltpu.VMEM((TOK, 2 * HEADS * HD), BF),
            pltpu.VMEM((SUB * 8, 128), F32), pltpu.VMEM((SUB * 8, 128), F32), pltpu.VMEM((SUB * 8, 128), F32),
            pltpu.VMEM((SUB * 8, 128), F32), pltpu.VMEM((SUB * 8, 128), F32),
            pltpu.VMEM((depth, cache_rows, HD), BF), pltpu.VMEM((depth, cache_rows, HD), BF),
            pltpu.VMEM((back, cache_rows, HD), BF), pltpu.VMEM((back, cache_rows, HD), BF),
            pltpu.SemaphoreType.DMA, pltpu.SemaphoreType.DMA((ring,)),
            pltpu.SemaphoreType.DMA((depth,)), pltpu.SemaphoreType.DMA((depth,)),
            pltpu.SemaphoreType.DMA((back,)), pltpu.SemaphoreType.DMA((back,)),
        ],
        compiler_params=pltpu.CompilerParams(vmem_limit_bytes=VMEM_BYTES),
        name="attention",
    )(x, gain, wkv, router_t, wq, kc, vc, ids, pos, cos_tab, sin_tab)


HALF = TOK // 2


class PairSum:
    def __init__(self, part_at, r1, cs, r2, fin, r3, sems):
        self.part_at, self.r1, self.cs, self.r2, self.fin, self.r3 = part_at, r1, cs, r2, fin, r3
        self.own_at = lambda j: part_at(j, self.own)
        self.sems = sems
        self.width = r1.shape[2]
        me = lax.axis_index("tp")
        chip, core = me // 2, me % 2
        self.sib = chip * 2 + (1 - core)
        self.peer = (1 - chip) * 2 + core
        self.own = pl.ds(pl.multiple_of(core * HALF, HALF), HALF)
        self.other = pl.ds(pl.multiple_of((1 - core) * HALF, HALF), HALF)

    def greet(self):
        barrier = pltpu.get_barrier_semaphore()
        for d in (self.sib, self.peer):
            pl.semaphore_signal(barrier, inc=1, device_id={"tp": d}, device_id_type=MESH)
        pl.semaphore_wait(barrier, 2)

    def cols(self, j):
        return pl.ds(pl.multiple_of(j * self.width, self.width), self.width)

    def copy(self, stage, j):
        src, dst, to = ((self.part_at(j, self.other), self.r1.at[j], self.sib),
                        (self.cs.at[j], self.r2.at[j], self.peer),
                        (self.fin.at[j], self.r3.at[j], self.sib))[stage]
        return pltpu.make_async_remote_copy(src, dst, self.sems.at[0, stage, j], self.sems.at[1, stage, j],
                                            device_id={"tp": to}, device_id_type=MESH)

    def first(self, j):
        self.copy(0, j).start()

    def second(self, j):
        self.copy(0, j).wait()
        self.cs[j] = (self.own_at(j)[...].astype(F32) + self.r1[j].astype(F32)).astype(BF)
        self.copy(1, j).start()

    def third(self, j, base_ref):
        self.copy(1, j).wait()
        both = self.cs[j].astype(F32) + self.r2[j].astype(F32)
        self.fin[j] = (base_ref[self.own, self.cols(j)].astype(F32) + both).astype(BF)
        self.copy(2, j).start()

    def last(self, j, out_ref):
        self.copy(2, j).wait()
        out_ref[self.own, self.cols(j)] = self.fin[j]
        out_ref[self.other, self.cols(j)] = self.r3[j]

    def finish(self, chunks, base_ref, out_ref):
        def step(j, _):
            self.third(j, base_ref)

            @pl.when(j >= 1)
            def _():
                self.last(j - 1, out_ref)
            return 0

        lax.fori_loop(0, chunks, step, 0)
        self.last(chunks - 1, out_ref)


def pair_scratch(chunks, width):
    return [pltpu.VMEM((chunks, HALF, width), BF)] * 5 + [pltpu.SemaphoreType.DMA((2, 3, chunks))]


def project_kernel(x_hbm, o_ref, meta_ref, wo_hbm, xm_ref, xv, wo, oe, gb, acc, x_sem, wo_sem, part, r1, cs, r2, fin, r3, sems):
    chunks, width = part.shape[0], part.shape[2]
    ring = wo.shape[0]
    half = HEADS * HD

    def wo_copy(j):
        return pltpu.make_async_copy(wo_hbm.at[:, :, pl.ds(pl.multiple_of(j * width, width), width)], wo.at[j % ring], wo_sem.at[j % ring])

    for j in range(ring):
        wo_copy(j).start()
    x_copy = pltpu.make_async_copy(x_hbm, xv, x_sem)
    x_copy.start()
    net = PairSum(lambda j, rows: part.at[j, rows], r1, cs, r2, fin, r3, sems)
    net.greet()

    id0, id1, g0, g1 = (jnp.broadcast_to(meta_ref[:, n:n + 1], (TOK, 128)) for n in range(4))

    def prepare(e):
        m0 = id0 == float(e)
        m1 = id1 == float(e)
        f0 = jnp.where(m0, 1.0, 0.0).astype(BF)
        f1 = jnp.where(m1, 1.0, 0.0).astype(BF)
        for n in range(HEADS):
            c = slice(n * HD, (n + 1) * HD)
            oe[e, :, c] = o_ref[:, c] * f0 + o_ref[:, half + n * HD:half + (n + 1) * HD] * f1
        gb[e] = jnp.where(m0, g0, jnp.where(m1, g1, 0.0))

    def project(j, fresh):
        wo_copy(j).wait()
        slot = j % ring
        for e in range(ATT_E):
            if fresh:
                prepare(e)
            prod = dot(oe[e], wo[slot, e])
            for n in range(width // 128):
                c = slice(n * 128, (n + 1) * 128)
                term = gb[e] * prod[:, c]
                if e == 0:
                    acc[:, c] = term
                elif e < ATT_E - 1:
                    acc[:, c] += term
                else:
                    part[j, :, c] = (acc[:, c] + term).astype(BF)
        net.first(j)

    def chunk_step(j, _):
        project(j, False)

        @pl.when(j + ring < chunks)
        def _():
            wo_copy(j + ring).start()

        @pl.when(j >= 2)
        def _():
            net.second(j - 1)
        return 0

    project(0, True)
    wo_copy(ring).start()
    net.second(0)
    lax.fori_loop(1, chunks, chunk_step, 0)
    net.second(chunks - 1)
    x_copy.wait()
    net.finish(chunks, xv, xm_ref)


def project_call(x, o, meta, wo):
    chunks = 8
    width = HID // chunks
    ring = 3
    return pl.pallas_call(
        project_kernel,
        out_shape=jax.ShapeDtypeStruct((TOK, HID), BF),
        in_specs=[hspec(), vspec(), vspec(), hspec()],
        out_specs=vspec(),
        scratch_shapes=[
            pltpu.VMEM((TOK, HID), BF),
            pltpu.VMEM((ring, ATT_E, HEADS * HD, width), BF),
            pltpu.VMEM((ATT_E, TOK, HEADS * HD), BF),
            pltpu.VMEM((ATT_E, TOK, 128), F32),
            pltpu.VMEM((TOK, width), F32),
            pltpu.SemaphoreType.DMA, pltpu.SemaphoreType.DMA((ring,)),
            pltpu.VMEM((chunks, TOK, width), BF),
        ] + pair_scratch(chunks, width),
        compiler_params=pltpu.CompilerParams(vmem_limit_bytes=VMEM_BYTES, collective_id=0, has_side_effects=True),
        name="project_sum",
    )(x, o, meta, wo)


FB = 512
NF = FFN // FB
DB = 512
ND = HID // DB
ROW_STEPS = (128, 160, 192, 256, 288, 320, 352, 384, 512)


def experts_kernel(xm_ref, gain_ref, router_ref, ids_ref, wg_hbm, wu_hbm, wd_hbm, y_ref,
                   u, pick, spread, xc, ac, gc, wg, wu, wd, count, wg_sem, wu_sem, wd_sem):
    ring = wg.shape[0]
    dring = wd.shape[0]
    steps = 2 * NF
    dsteps = 2 * ND
    first_id = lax.axis_index("tp") * 2

    def in_copies(t):
        f = pl.ds(pl.multiple_of((t // 2) * FB, FB), FB)
        s = t % ring
        return (pltpu.make_async_copy(wg_hbm.at[t % 2, :, f], wg.at[s], wg_sem.at[s]),
                pltpu.make_async_copy(wu_hbm.at[t % 2, :, f], wu.at[s], wu_sem.at[s]))

    def down_copy(t):
        c = pl.ds(pl.multiple_of((t // 2) * DB, DB), DB)
        return pltpu.make_async_copy(wd_hbm.at[t % 2, :, c], wd.at[t % dring], wd_sem.at[t % dring])

    for t in range(ring):
        for c in in_copies(t):
            c.start()

    gain = gain_ref[...]

    def norm_step(i, _):
        r = pl.ds(pl.multiple_of(i * 64, 64), 64)
        u[r, :] = norm_rows(xm_ref[r, :], gain)
        return 0

    lax.fori_loop(0, TOK // 64, norm_step, 0)
    cols = columns_of(ids_ref[...])
    id0, id1 = cols[:, 0:1], cols[:, 1:2]
    logits = dot_nt(u[...], router_ref[...])
    g0, g1 = pair_gates(logits, id0, id1)
    lane = lax.broadcasted_iota(jnp.int32, (TOK, 128), 1)
    mine = (lane + first_id).astype(F32)
    gates = jnp.where(mine == id0, g0, jnp.where(mine == id1, g1, 0.0)).T

    row = lax.broadcasted_iota(jnp.int32, (TOK, TOK), 0)
    before = (row < lax.broadcasted_iota(jnp.int32, (TOK, TOK), 1)).astype(F32).astype(BF)
    for e in range(2):
        target = first_id + e
        hit = ((ids_ref[0:1, :] == target) | (ids_ref[1:2, :] == target)).astype(F32)
        rank = dot(jnp.broadcast_to(hit, (8, TOK)).astype(BF), before)[0:1, :]
        place = jnp.where(hit > 0.5, rank, -1.0)
        sel = (row.astype(F32) == place).astype(F32)
        pick[...] = sel.astype(BF)
        spread[e] = sel.T.astype(BF)
        gc[e] = jnp.broadcast_to(jnp.sum(sel * gates[e:e + 1, :], axis=1, keepdims=True), (TOK, 128))
        xc[e] = dot(pick[...], u[...]).astype(BF)
        count[e] = (jnp.sum(hit).astype(jnp.int32) + 31) // 32

    def by_blocks(blocks, run):
        for low, high in zip((0,) + ROW_STEPS[:-1], ROW_STEPS):
            @pl.when((blocks * 32 > low) & (blocks * 32 <= high) if low else blocks * 32 <= high)
            def _(high=high):
                run(high)

    def block_step(t, _):
        e = t % 2
        s = t % ring
        f = pl.ds(pl.multiple_of((t // 2) * FB, FB), FB)
        for c in in_copies(t):
            c.wait()

        def run(m):
            g = dot(xc[e, 0:m, :], wg[s])
            up = dot(xc[e, 0:m, :], wu[s])
            ac[e, 0:m, f] = (jax.nn.silu(g) * up).astype(BF)

        by_blocks(count[e], run)

        @pl.when(t + ring < steps)
        def _():
            for c in in_copies(t + ring):
                c.start()

        @pl.when((t + ring >= steps) & (t + ring < steps + dring))
        def _():
            down_copy(t + ring - steps).start()
        return 0

    lax.fori_loop(0, steps, block_step, 0)

    def down_step(t, _):
        e = t % 2
        s = t % dring
        c = pl.ds(pl.multiple_of((t // 2) * DB, DB), DB)
        down_copy(t).wait()

        def run(m):
            d = dot(ac[e, 0:m, :], wd[s])
            gate = gc[e, 0:m, :]
            parts = [(d[:, n * 128:(n + 1) * 128] * gate).astype(BF) for n in range(DB // 128)]
            back = dot(spread[e, :, 0:m], jnp.concatenate(parts, axis=1))
            y_ref[:, c] = (jnp.where(e == 0, 0.0, y_ref[:, c].astype(F32)) + back).astype(BF)

        by_blocks(count[e], run)

        @pl.when(t + dring < dsteps)
        def _():
            down_copy(t + dring).start()
        return 0

    lax.fori_loop(0, dsteps, down_step, 0)


def experts_call(xm, gain, router_t, ids, wg, wu, wd):
    ring = 4
    dring = 3
    return pl.pallas_call(
        experts_kernel,
        out_shape=jax.ShapeDtypeStruct((TOK, HID), BF),
        in_specs=[vspec(), vspec(), vspec(), vspec(), hspec(), hspec(), hspec()],
        out_specs=vspec(),
        scratch_shapes=[
            pltpu.VMEM((TOK, HID), BF), pltpu.VMEM((TOK, TOK), BF), pltpu.VMEM((2, TOK, TOK), BF), pltpu.VMEM((2, TOK, HID), BF),
            pltpu.VMEM((2, TOK, FFN), BF), pltpu.VMEM((2, TOK, 128), F32),
            pltpu.VMEM((ring, HID, FB), BF), pltpu.VMEM((ring, HID, FB), BF), pltpu.VMEM((dring, FFN, DB), BF),
            pltpu.SMEM((2,), jnp.int32),
            pltpu.SemaphoreType.DMA((ring,)), pltpu.SemaphoreType.DMA((ring,)), pltpu.SemaphoreType.DMA((dring,)),
        ],
        compiler_params=pltpu.CompilerParams(vmem_limit_bytes=VMEM_BYTES),
        name="experts",
    )(xm, gain, router_t, ids, wg, wu, wd)


def sum_kernel(xm_hbm, y_hbm, out_ref, xv, yv, in_sem, r1, cs, r2, fin, r3, sems):
    chunks, width = r1.shape[0], r1.shape[2]

    def y_at(j, rows):
        return y_hbm.at[rows, pl.ds(pl.multiple_of(j * width, width), width)]

    net = PairSum(y_at, r1, cs, r2, fin, r3, sems)
    x_copy = pltpu.make_async_copy(xm_hbm.at[net.own], xv.at[net.own], in_sem.at[0])
    y_copy = pltpu.make_async_copy(y_hbm.at[net.own], yv.at[net.own], in_sem.at[1])
    y_copy.start()
    x_copy.start()
    net.greet()
    for j in range(chunks):
        net.first(j)
    y_copy.wait()
    net.own_at = lambda j: yv.at[net.own, net.cols(j)]

    def step(j, _):
        net.second(j)
        return 0

    lax.fori_loop(0, chunks, step, 0)
    x_copy.wait()
    net.finish(chunks, xv, out_ref)


def sum_call(xm, y):
    chunks = 8
    width = HID // chunks
    return pl.pallas_call(
        sum_kernel,
        out_shape=pltpu.VMEM((TOK, HID), BF),
        in_specs=[hspec(), hspec()],
        out_specs=vspec(),
        scratch_shapes=[pltpu.VMEM((TOK, HID), BF), pltpu.VMEM((TOK, HID), BF), pltpu.SemaphoreType.DMA((2,))] + pair_scratch(chunks, width),
        compiler_params=pltpu.CompilerParams(vmem_limit_bytes=57 * 1024 * 1024, collective_id=1, has_side_effects=True),
        name="expert_sum",
    )(xm, y)


def rope_tables():
    inv_freq = np.power(np.float64(ROPE_BASE), -(np.arange(HD // 2) * 2.0 / HD))
    angle = (np.arange(SLOTS, dtype=np.float32)[:, None] * inv_freq.astype(np.float32)[None, :]).astype(np.float64)
    cos = np.cos(angle).astype(np.float32)
    sin = np.sin(angle).astype(np.float32)
    return np.concatenate([cos, cos], axis=1), np.concatenate([-sin, sin], axis=1)


def solution(mesh):
    cos_tab, sin_tab = rope_tables()

    def local_step(x, k_cache, v_cache, positions, att_ids, mlp_ids, norm_att, w_kv, router_att, w_query, w_out, norm_mlp, router_mlp, w_gate, w_up, w_down):
        flat = (TOK * SLOTS * HEADS, HD)
        wkv = w_kv.reshape(HID, HEADS, 2, HD).transpose(0, 2, 1, 3).reshape(HID * 2 * HEADS, HD)
        k_out, v_out, o, meta = attention_call(
            x, norm_att[None, :], wkv, router_att.T, w_query, k_cache.reshape(flat), v_cache.reshape(flat), att_ids.T, positions[None, :],
            jnp.asarray(cos_tab), jnp.asarray(sin_tab))
        xm = project_call(x, o, meta, w_out)
        y = experts_call(xm, norm_mlp[None, :], router_mlp.T, mlp_ids.T, w_gate, w_up, w_down)
        x_out = sum_call(xm, y)
        return x_out, k_out.reshape(k_cache.shape), v_out.reshape(v_cache.shape)

    token_spec = P('dp', None)
    cache_spec = P('dp', None, 'tp', None)
    expert_spec = P('tp', None, None)
    in_specs = (token_spec, cache_spec, cache_spec, P('dp'), token_spec, token_spec, P(), P(None, 'tp', None), P(), P(None, None, 'tp'), P(None, 'tp', None), P(), P(), expert_spec, expert_spec, expert_spec)
    out_specs = (token_spec, cache_spec, cache_spec)
    return jax.shard_map(local_step, mesh=mesh, in_specs=in_specs, out_specs=out_specs, check_vma=False)
```

```python
import functools

import jax
import jax.numpy as jnp
import numpy as np
from jax import lax
from jax.experimental import pallas as pl
from jax.experimental.pallas import tpu as pltpu
from jax.sharding import PartitionSpec as P

NORM_EPS = 1e-6
ROPE_BASE = 10000.0
BF = jnp.bfloat16
F32 = jnp.float32
MESH = pl.DeviceIdType.MESH
VMEM_BYTES = 62 * 1024 * 1024

TOK = 512
HID = 2048
HEADS = 4
HD = 128
SLOTS = 16
ATT_E = 8
FFN = 5632
SUB = 64


def vspec():
    return pl.BlockSpec(memory_space=pltpu.VMEM)


def hspec():
    return pl.BlockSpec(memory_space=pl.ANY)


def dot(a, b):
    return jnp.dot(a, b, preferred_element_type=F32)


def dot_nt(a, b):
    return lax.dot_general(a, b, (((1,), (1,)), ((), ())), preferred_element_type=F32)


def norm_rows(x, gain):
    v = x.astype(F32)
    inv = lax.rsqrt(jnp.mean(v * v, axis=-1, keepdims=True) + NORM_EPS)
    return (v * inv * gain).astype(BF)


def columns_of(rows):
    pad = jnp.zeros((128 - rows.shape[0], TOK), F32)
    return jnp.concatenate([rows.astype(F32), pad], axis=0).T


def pair_gates(logits, id0, id1):
    lane = lax.broadcasted_iota(jnp.int32, logits.shape, 1).astype(F32)
    l0 = jnp.sum(jnp.where(lane == id0, logits, 0.0), axis=1, keepdims=True)
    l1 = jnp.sum(jnp.where(lane == id1, logits, 0.0), axis=1, keepdims=True)
    top = jnp.maximum(l0, l1)
    e0 = jnp.exp(l0 - top)
    e1 = jnp.exp(l1 - top)
    total = e0 + e1
    return e0 / total, e1 / total


def attention_kernel(x_ref, gain_ref, wkv_hbm, router_ref, wq_hbm, kc_hbm, vc_hbm, ids_ref, pos_ref, cos_ref, sin_ref,
                     ko_hbm, vo_hbm, o_ref, meta_ref,
                     h, wkv_raw, wkv_wide, wkv, wq, cosb, sinb, qf, kvb, qb, q8, kn8, vn8, pos8, o8, kin, vin, kout, vout,
                     wkv_sem, wq_sem, kin_sem, vin_sem, ko_sem, vo_sem):
    ring = wq.shape[0]
    steps = TOK // SUB
    depth = kin.shape[0]
    back = kout.shape[0]
    cache_rows = SUB * SLOTS * HEADS

    def cache_rows_at(i):
        return pl.ds(pl.multiple_of(i * cache_rows, cache_rows), cache_rows)

    def wq_copy(e):
        return pltpu.make_async_copy(wq_hbm.at[e], wq.at[e % ring], wq_sem.at[e % ring])

    def in_copies(i):
        s = i % depth
        return (pltpu.make_async_copy(kc_hbm.at[cache_rows_at(i)], kin.at[s], kin_sem.at[s]),
                pltpu.make_async_copy(vc_hbm.at[cache_rows_at(i)], vin.at[s], vin_sem.at[s]))

    def out_copies(i):
        s = i % back
        return (pltpu.make_async_copy(kout.at[s], ko_hbm.at[cache_rows_at(i)], ko_sem.at[s]),
                pltpu.make_async_copy(vout.at[s], vo_hbm.at[cache_rows_at(i)], vo_sem.at[s]))

    wkv_copy = pltpu.make_async_copy(wkv_hbm, wkv_raw, wkv_sem)
    wq_copy(0).start()
    wkv_copy.start()
    for e in range(1, ring):
        wq_copy(e).start()

    gain = gain_ref[...]

    def norm_step(i, _):
        r = pl.ds(pl.multiple_of(i * 64, 64), 64)
        h[r, :] = norm_rows(x_ref[r, :], gain)
        return 0

    lax.fori_loop(0, TOK // 64, norm_step, 0)

    cols = columns_of(jnp.concatenate([ids_ref[...], pos_ref[...]], axis=0))
    id0, id1, pos = cols[:, 0:1], cols[:, 1:2], cols[:, 2:3]
    logits = dot_nt(h[...], router_ref[...])
    g0, g1 = pair_gates(logits, id0, id1)
    lane = lax.broadcasted_iota(jnp.int32, (TOK, 128), 1)
    meta_ref[...] = jnp.where(lane == 0, id0, jnp.where(lane == 1, id1, jnp.where(lane == 2, g0, jnp.where(lane == 3, g1, pos))))

    cb = jnp.zeros((TOK, HD), F32)
    sb = jnp.zeros((TOK, HD), F32)
    for p in range(SLOTS):
        hit = pos == float(p)
        cb = jnp.where(hit, cos_ref[p:p + 1, :], cb)
        sb = jnp.where(hit, sin_ref[p:p + 1, :], sb)
    cosb[...] = cb
    sinb[...] = sb

    def rope(v):
        return v * cosb[...] + pltpu.roll(v, HD // 2, 1) * sinb[...]

    wkv_copy.wait()
    half = HEADS * HD
    deep = HID // ATT_E

    def query_step(e, _):
        wq_copy(e).wait()

        @pl.when(e < depth)
        def _():
            for c in in_copies(e):
                c.start()
        ef = e.astype(F32)
        qe = dot(h[...], wq[e % ring])
        m0 = meta_ref[:, 0:1] == ef
        m1 = meta_ref[:, 1:2] == ef
        qf[:, 0:half] = jnp.where(m0, qe, qf[:, 0:half])
        qf[:, half:2 * half] = jnp.where(m1, qe, qf[:, half:2 * half])
        wkv_wide[...] = wkv_raw[pl.ds(pl.multiple_of(e * deep * 8, deep * 8), deep * 8), :].astype(F32)
        for j in range(8):
            wkv[pl.ds(pl.multiple_of(e * deep, deep), deep), j * HD:(j + 1) * HD] = wkv_wide[pl.ds(j, deep, stride=8), :].astype(BF)

        @pl.when(e + ring < ATT_E)
        def _():
            wq_copy(e + ring).start()
        return 0

    lax.fori_loop(0, ATT_E, query_step, 0)
    kf = dot(h[...], wkv[:, 0:half])
    for n in range(HEADS):
        kvb[:, n * HD:(n + 1) * HD] = rope(kf[:, n * HD:(n + 1) * HD]).astype(BF)
    kvb[:, half:2 * half] = dot(h[...], wkv[:, half:2 * half]).astype(BF)
    for n in range(2 * HEADS):
        c = slice(n * HD, (n + 1) * HD)
        qb[:, c] = rope(qf[:, c]).astype(BF)

    group = 4
    rows = group * 2 * HEADS
    lane32 = lax.broadcasted_iota(jnp.int32, (rows, 128), 1)
    row32 = lax.broadcasted_iota(jnp.int32, (rows, 128), 0)
    own_part = ((lane32 // 64) == ((row32 // 8) % 2)) & ((lane32 % 4) == (row32 % 4))
    slot32 = ((lane32 // 4) % 16).astype(F32)
    slot_id = (2 * lax.broadcasted_iota(jnp.int32, (8, 8, 128), 0) + lax.broadcasted_iota(jnp.int32, (8, 8, 128), 1) // 4).astype(F32)
    scale = HD ** -0.5
    upper = row32 < rows // 2

    def cache_step(i, _):
        s = i % depth
        so = i % back
        r = pl.ds(pl.multiple_of(i * SUB, SUB), SUB)
        for j in range(2 * HEADS):
            q8[pl.ds(j, SUB, stride=8), :] = qb[r, j * HD:(j + 1) * HD].astype(F32)
            n = j % HEADS
            kn8[pl.ds(j, SUB, stride=8), :] = kvb[r, n * HD:(n + 1) * HD].astype(F32)
            vn8[pl.ds(j, SUB, stride=8), :] = kvb[r, half + n * HD:half + (n + 1) * HD].astype(F32)
            pos8[pl.ds(j, SUB, stride=8), :] = jnp.broadcast_to(meta_ref[r, 4:5], (SUB, 128))

        @pl.when(i >= back)
        def _():
            for c in out_copies(i - back):
                c.wait()
        for c in in_copies(i):
            c.wait()

        def group_rows(g):
            return slice(g * group * 64, (g + 1) * group * 64), slice(g * group * 8, (g + 1) * group * 8)

        for part in range(SUB // 32):
            groups = range(part * 8, part * 8 + 8, 2)
            scores = []
            for g0 in groups:
                keys, queries = [], []
                for g in (g0, g0 + 1):
                    rr, r8 = group_rows(g)
                    hit = slot_id[None] == pos8[r8, :].reshape(group, 1, 8, 128)
                    old_k = kin[s, rr, :].astype(F32).reshape(group, 8, 8, 128)
                    new_k = jnp.where(hit, kn8[r8, :].reshape(group, 1, 8, 128), old_k).reshape(group * 64, 128).astype(BF)
                    kout[so, rr, :] = new_k
                    old_v = vin[s, rr, :].astype(F32).reshape(group, 8, 8, 128)
                    new_v = jnp.where(hit, vn8[r8, :].reshape(group, 1, 8, 128), old_v).reshape(group * 64, 128).astype(BF)
                    vout[so, rr, :] = new_v
                    keys.append(new_k)
                    queries.append(q8[r8, :].astype(BF))
                none = jnp.zeros((rows, 128), BF)
                both = jnp.concatenate([jnp.concatenate([queries[0], none], axis=1), jnp.concatenate([none, queries[1]], axis=1)], axis=0)
                sc = dot_nt(both, jnp.concatenate(keys, axis=1))
                for b in (0, rows):
                    scores.append(jnp.concatenate([sc[b:b + rows // 2, 0:128], sc[b + rows // 2:b + rows, 128:256]], axis=0))
            for n, g0 in enumerate(groups):
                wides, values = [], []
                for b in range(2):
                    rr, r8 = group_rows(g0 + b)
                    valid = own_part & (slot32 <= pos8[r8, :])
                    sc = jnp.where(valid, scores[2 * n + b] * scale, -1e30)
                    ex = jnp.exp(sc - jnp.max(sc, axis=1, keepdims=True))
                    w = ex / jnp.sum(ex, axis=1, keepdims=True)
                    wides.append(jnp.concatenate([jnp.where(upper, w, 0.0), jnp.where(upper, 0.0, w)], axis=1).astype(BF))
                    values.append(vout[so, rr, :])
                res = dot(jnp.concatenate(wides, axis=0), jnp.concatenate(values, axis=1))
                for b in range(2):
                    o8[group_rows(g0 + b)[1], :] = res[b * rows:(b + 1) * rows, b * 128:(b + 1) * 128]

        for c in out_copies(i):
            c.start()

        @pl.when(i + depth < steps)
        def _():
            for c in in_copies(i + depth):
                c.start()
        for j in range(2 * HEADS):
            o_ref[r, j * HD:(j + 1) * HD] = o8[pl.ds(j, SUB, stride=8), :].astype(BF)
        return 0

    lax.fori_loop(0, steps, cache_step, 0)
    for i in range(steps - back, steps):
        for c in out_copies(i):
            c.wait()


def attention_call(x, gain, wkv, router_t, wq, kc, vc, ids, pos, cos_tab, sin_tab):
    ring = 4
    depth = 4
    back = 2
    cache_rows = SUB * SLOTS * HEADS
    cache = jax.ShapeDtypeStruct(kc.shape, BF)
    return pl.pallas_call(
        attention_kernel,
        out_shape=(cache, cache, jax.ShapeDtypeStruct((TOK, 2 * HEADS * HD), BF), jax.ShapeDtypeStruct((TOK, 128), F32)),
        in_specs=[vspec(), vspec(), hspec(), vspec(), hspec(), hspec(), hspec(), vspec(), vspec(), vspec(), vspec()],
        out_specs=(hspec(), hspec(), vspec(), vspec()),
        scratch_shapes=[
            pltpu.VMEM((TOK, HID), BF),
            pltpu.VMEM(wkv.shape, BF), pltpu.VMEM((2048, HD), F32), pltpu.VMEM((HID, 2 * HEADS * HD), BF),
            pltpu.VMEM((ring,) + wq.shape[1:], BF),
            pltpu.VMEM((TOK, HD), F32), pltpu.VMEM((TOK, HD), F32),
            pltpu.VMEM((TOK, 2 * HEADS * HD), F32),
            pltpu.VMEM((TOK, 2 * HEADS * HD), BF),
            pltpu.VMEM((TOK, 2 * HEADS * HD), BF),
            pltpu.VMEM((SUB * 8, 128), F32), pltpu.VMEM((SUB * 8, 128), F32), pltpu.VMEM((SUB * 8, 128), F32),
            pltpu.VMEM((SUB * 8, 128), F32), pltpu.VMEM((SUB * 8, 128), F32),
            pltpu.VMEM((depth, cache_rows, HD), BF), pltpu.VMEM((depth, cache_rows, HD), BF),
            pltpu.VMEM((back, cache_rows, HD), BF), pltpu.VMEM((back, cache_rows, HD), BF),
            pltpu.SemaphoreType.DMA, pltpu.SemaphoreType.DMA((ring,)),
            pltpu.SemaphoreType.DMA((depth,)), pltpu.SemaphoreType.DMA((depth,)),
            pltpu.SemaphoreType.DMA((back,)), pltpu.SemaphoreType.DMA((back,)),
        ],
        compiler_params=pltpu.CompilerParams(vmem_limit_bytes=VMEM_BYTES),
        name="attention",
    )(x, gain, wkv, router_t, wq, kc, vc, ids, pos, cos_tab, sin_tab)


HALF = TOK // 2


class PairSum:
    def __init__(self, part_at, r1, cs, r2, fin, r3, sems):
        self.part_at, self.r1, self.cs, self.r2, self.fin, self.r3 = part_at, r1, cs, r2, fin, r3
        self.own_at = lambda j: part_at(j, self.own)
        self.sems = sems
        self.width = r1.shape[2]
        me = lax.axis_index("tp")
        chip, core = me // 2, me % 2
        self.sib = chip * 2 + (1 - core)
        self.peer = (1 - chip) * 2 + core
        self.own = pl.ds(pl.multiple_of(core * HALF, HALF), HALF)
        self.other = pl.ds(pl.multiple_of((1 - core) * HALF, HALF), HALF)

    def greet(self):
        barrier = pltpu.get_barrier_semaphore()
        for d in (self.sib, self.peer):
            pl.semaphore_signal(barrier, inc=1, device_id={"tp": d}, device_id_type=MESH)

    def meet(self):
        pl.semaphore_wait(pltpu.get_barrier_semaphore(), 2)

    def cols(self, j):
        return pl.ds(pl.multiple_of(j * self.width, self.width), self.width)

    def copy(self, stage, j):
        src, dst, to = ((self.part_at(j, self.other), self.r1.at[j], self.sib),
                        (self.cs.at[j], self.r2.at[j], self.peer),
                        (self.fin.at[j], self.r3.at[j], self.sib))[stage]
        return pltpu.make_async_remote_copy(src, dst, self.sems.at[0, stage, j], self.sems.at[1, stage, j],
                                            device_id={"tp": to}, device_id_type=MESH)

    def first(self, j):
        self.copy(0, j).start()

    def second(self, j):
        self.copy(0, j).wait()
        self.cs[j] = (self.own_at(j)[...].astype(F32) + self.r1[j].astype(F32)).astype(BF)
        self.copy(1, j).start()

    def third(self, j, base_ref):
        self.copy(1, j).wait()
        both = self.cs[j].astype(F32) + self.r2[j].astype(F32)
        self.fin[j] = (base_ref[self.own, self.cols(j)].astype(F32) + both).astype(BF)
        self.copy(2, j).start()

    def last(self, j, out_ref):
        self.copy(2, j).wait()
        out_ref[self.own, self.cols(j)] = self.fin[j]
        out_ref[self.other, self.cols(j)] = self.r3[j]

    def finish(self, chunks, base_ref, out_ref):
        def step(j, _):
            self.third(j, base_ref)

            @pl.when(j >= 1)
            def _():
                self.last(j - 1, out_ref)
            return 0

        lax.fori_loop(0, chunks, step, 0)
        self.last(chunks - 1, out_ref)


def pair_scratch(chunks, width):
    return [pltpu.VMEM((chunks, HALF, width), BF)] * 5 + [pltpu.SemaphoreType.DMA((2, 3, chunks))]


def project_kernel(x_hbm, o_ref, meta_ref, wo_hbm, xm_ref, xv, wo, oe, gb, acc, x_sem, wo_sem, part, r1, cs, r2, fin, r3, sems):
    chunks, width = part.shape[0], part.shape[2]
    ring = wo.shape[0]
    half = HEADS * HD

    def wo_copy(j):
        return pltpu.make_async_copy(wo_hbm.at[:, :, pl.ds(pl.multiple_of(j * width, width), width)], wo.at[j % ring], wo_sem.at[j % ring])

    for j in range(ring):
        wo_copy(j).start()
    x_copy = pltpu.make_async_copy(x_hbm, xv, x_sem)
    x_copy.start()
    net = PairSum(lambda j, rows: part.at[j, rows], r1, cs, r2, fin, r3, sems)
    net.greet()

    id0, id1, g0, g1 = (jnp.broadcast_to(meta_ref[:, n:n + 1], (TOK, 128)) for n in range(4))

    def prepare(e):
        m0 = id0 == float(e)
        m1 = id1 == float(e)
        f0 = jnp.where(m0, 1.0, 0.0).astype(BF)
        f1 = jnp.where(m1, 1.0, 0.0).astype(BF)
        for n in range(HEADS):
            c = slice(n * HD, (n + 1) * HD)
            oe[e, :, c] = o_ref[:, c] * f0 + o_ref[:, half + n * HD:half + (n + 1) * HD] * f1
        gb[e] = jnp.where(m0, g0, jnp.where(m1, g1, 0.0))

    def project(j, fresh):
        wo_copy(j).wait()
        slot = j % ring
        for e in range(ATT_E):
            prod = dot(oe[e], wo[slot, e])
            for n in range(width // 128):
                c = slice(n * 128, (n + 1) * 128)
                term = gb[e] * prod[:, c]
                if e == 0:
                    acc[:, c] = term
                elif e < ATT_E - 1:
                    acc[:, c] += term
                else:
                    part[j, :, c] = (acc[:, c] + term).astype(BF)
        if fresh:
            net.meet()
        net.first(j)

    def chunk_step(j, _):
        project(j, False)

        @pl.when(j + ring < chunks)
        def _():
            wo_copy(j + ring).start()

        @pl.when(j >= 2)
        def _():
            net.second(j - 1)
        return 0

    for e in range(ATT_E):
        prepare(e)
    project(0, True)
    wo_copy(ring).start()
    net.second(0)
    lax.fori_loop(1, chunks, chunk_step, 0)
    net.second(chunks - 1)
    x_copy.wait()
    net.finish(chunks, xv, xm_ref)


def project_call(x, o, meta, wo):
    chunks = 8
    width = HID // chunks
    ring = 3
    return pl.pallas_call(
        project_kernel,
        out_shape=jax.ShapeDtypeStruct((TOK, HID), BF),
        in_specs=[hspec(), vspec(), vspec(), hspec()],
        out_specs=vspec(),
        scratch_shapes=[
            pltpu.VMEM((TOK, HID), BF),
            pltpu.VMEM((ring, ATT_E, HEADS * HD, width), BF),
            pltpu.VMEM((ATT_E, TOK, HEADS * HD), BF),
            pltpu.VMEM((ATT_E, TOK, 128), F32),
            pltpu.VMEM((TOK, width), F32),
            pltpu.SemaphoreType.DMA, pltpu.SemaphoreType.DMA((ring,)),
            pltpu.VMEM((chunks, TOK, width), BF),
        ] + pair_scratch(chunks, width),
        compiler_params=pltpu.CompilerParams(vmem_limit_bytes=VMEM_BYTES, collective_id=0, has_side_effects=True),
        name="project_sum",
    )(x, o, meta, wo)


FB = 512
NF = FFN // FB
DB = 512
ND = HID // DB
ROW_STEPS = (128, 160, 192, 256, 288, 320, 352, 384, 512)


def experts_kernel(xm_ref, gain_ref, router_ref, ids_ref, wg_hbm, wu_hbm, wd_hbm, y_ref,
                   u, pick, spread, xc, ac, gc, wg, wu, wd, count, wg_sem, wu_sem, wd_sem):
    ring = wg.shape[0]
    dring = wd.shape[0]
    steps = 2 * NF
    dsteps = 2 * ND
    first_id = lax.axis_index("tp") * 2

    def in_copies(t):
        f = pl.ds(pl.multiple_of((t // 2) * FB, FB), FB)
        s = t % ring
        return (pltpu.make_async_copy(wg_hbm.at[t % 2, :, f], wg.at[s], wg_sem.at[s]),
                pltpu.make_async_copy(wu_hbm.at[t % 2, :, f], wu.at[s], wu_sem.at[s]))

    def down_copy(t):
        c = pl.ds(pl.multiple_of((t // 2) * DB, DB), DB)
        return pltpu.make_async_copy(wd_hbm.at[t % 2, :, c], wd.at[t % dring], wd_sem.at[t % dring])

    for t in range(ring):
        for c in in_copies(t):
            c.start()

    gain = gain_ref[...]

    def norm_step(i, _):
        r = pl.ds(pl.multiple_of(i * 64, 64), 64)
        u[r, :] = norm_rows(xm_ref[r, :], gain)
        return 0

    lax.fori_loop(0, TOK // 64, norm_step, 0)
    cols = columns_of(ids_ref[...])
    id0, id1 = cols[:, 0:1], cols[:, 1:2]
    logits = dot_nt(u[...], router_ref[...])
    g0, g1 = pair_gates(logits, id0, id1)
    lane = lax.broadcasted_iota(jnp.int32, (TOK, 128), 1)
    mine = (lane + first_id).astype(F32)
    gates = jnp.where(mine == id0, g0, jnp.where(mine == id1, g1, 0.0)).T

    row = lax.broadcasted_iota(jnp.int32, (TOK, TOK), 0)
    before = (row < lax.broadcasted_iota(jnp.int32, (TOK, TOK), 1)).astype(F32).astype(BF)
    for e in range(2):
        target = first_id + e
        hit = ((ids_ref[0:1, :] == target) | (ids_ref[1:2, :] == target)).astype(F32)
        rank = dot(jnp.broadcast_to(hit, (8, TOK)).astype(BF), before)[0:1, :]
        place = jnp.where(hit > 0.5, rank, -1.0)
        sel = (row.astype(F32) == place).astype(F32)
        pick[...] = sel.astype(BF)
        spread[e] = sel.T.astype(BF)
        gc[e] = jnp.broadcast_to(jnp.sum(sel * gates[e:e + 1, :], axis=1, keepdims=True), (TOK, 128))
        xc[e] = dot(pick[...], u[...]).astype(BF)
        count[e] = (jnp.sum(hit).astype(jnp.int32) + 31) // 32

    def by_blocks(blocks, run):
        for low, high in zip((0,) + ROW_STEPS[:-1], ROW_STEPS):
            @pl.when((blocks * 32 > low) & (blocks * 32 <= high) if low else blocks * 32 <= high)
            def _(high=high):
                run(high)

    def block_step(t, _):
        e = t % 2
        s = t % ring
        f = pl.ds(pl.multiple_of((t // 2) * FB, FB), FB)
        for c in in_copies(t):
            c.wait()

        def run(m):
            g = dot(xc[e, 0:m, :], wg[s])
            up = dot(xc[e, 0:m, :], wu[s])
            ac[e, 0:m, f] = (jax.nn.silu(g) * up).astype(BF)

        by_blocks(count[e], run)

        @pl.when(t + ring < steps)
        def _():
            for c in in_copies(t + ring):
                c.start()

        @pl.when((t + ring >= steps) & (t + ring < steps + dring))
        def _():
            down_copy(t + ring - steps).start()
        return 0

    lax.fori_loop(0, steps, block_step, 0)

    def down_step(t, _):
        e = t % 2
        s = t % dring
        c = pl.ds(pl.multiple_of((t // 2) * DB, DB), DB)
        down_copy(t).wait()

        def run(m):
            d = dot(ac[e, 0:m, :], wd[s])
            gate = gc[e, 0:m, :]
            parts = [(d[:, n * 128:(n + 1) * 128] * gate).astype(BF) for n in range(DB // 128)]
            back = dot(spread[e, :, 0:m], jnp.concatenate(parts, axis=1))
            y_ref[:, c] = (jnp.where(e == 0, 0.0, y_ref[:, c].astype(F32)) + back).astype(BF)

        by_blocks(count[e], run)

        @pl.when(t + dring < dsteps)
        def _():
            down_copy(t + dring).start()
        return 0

    lax.fori_loop(0, dsteps, down_step, 0)


def experts_call(xm, gain, router_t, ids, wg, wu, wd):
    ring = 4
    dring = 3
    return pl.pallas_call(
        experts_kernel,
        out_shape=jax.ShapeDtypeStruct((TOK, HID), BF),
        in_specs=[vspec(), vspec(), vspec(), vspec(), hspec(), hspec(), hspec()],
        out_specs=vspec(),
        scratch_shapes=[
            pltpu.VMEM((TOK, HID), BF), pltpu.VMEM((TOK, TOK), BF), pltpu.VMEM((2, TOK, TOK), BF), pltpu.VMEM((2, TOK, HID), BF),
            pltpu.VMEM((2, TOK, FFN), BF), pltpu.VMEM((2, TOK, 128), F32),
            pltpu.VMEM((ring, HID, FB), BF), pltpu.VMEM((ring, HID, FB), BF), pltpu.VMEM((dring, FFN, DB), BF),
            pltpu.SMEM((2,), jnp.int32),
            pltpu.SemaphoreType.DMA((ring,)), pltpu.SemaphoreType.DMA((ring,)), pltpu.SemaphoreType.DMA((dring,)),
        ],
        compiler_params=pltpu.CompilerParams(vmem_limit_bytes=VMEM_BYTES),
        name="experts",
    )(xm, gain, router_t, ids, wg, wu, wd)


def sum_kernel(xm_hbm, y_hbm, out_ref, xv, yv, in_sem, r1, cs, r2, fin, r3, sems):
    chunks, width = r1.shape[0], r1.shape[2]

    def y_at(j, rows):
        return y_hbm.at[rows, pl.ds(pl.multiple_of(j * width, width), width)]

    net = PairSum(y_at, r1, cs, r2, fin, r3, sems)
    x_copy = pltpu.make_async_copy(xm_hbm.at[net.own], xv.at[net.own], in_sem.at[0])
    y_copy = pltpu.make_async_copy(y_hbm.at[net.own], yv.at[net.own], in_sem.at[1])
    y_copy.start()
    x_copy.start()
    net.greet()
    net.meet()
    for j in range(chunks):
        net.first(j)
    y_copy.wait()
    net.own_at = lambda j: yv.at[net.own, net.cols(j)]

    def step(j, _):
        net.second(j)
        return 0

    lax.fori_loop(0, chunks, step, 0)
    x_copy.wait()
    net.finish(chunks, xv, out_ref)


def sum_call(xm, y):
    chunks = 8
    width = HID // chunks
    return pl.pallas_call(
        sum_kernel,
        out_shape=pltpu.VMEM((TOK, HID), BF),
        in_specs=[hspec(), hspec()],
        out_specs=vspec(),
        scratch_shapes=[pltpu.VMEM((TOK, HID), BF), pltpu.VMEM((TOK, HID), BF), pltpu.SemaphoreType.DMA((2,))] + pair_scratch(chunks, width),
        compiler_params=pltpu.CompilerParams(vmem_limit_bytes=57 * 1024 * 1024, collective_id=1, has_side_effects=True),
        name="expert_sum",
    )(xm, y)


def rope_tables():
    inv_freq = np.power(np.float64(ROPE_BASE), -(np.arange(HD // 2) * 2.0 / HD))
    angle = (np.arange(SLOTS, dtype=np.float32)[:, None] * inv_freq.astype(np.float32)[None, :]).astype(np.float64)
    cos = np.cos(angle).astype(np.float32)
    sin = np.sin(angle).astype(np.float32)
    return np.concatenate([cos, cos], axis=1), np.concatenate([-sin, sin], axis=1)


def solution(mesh):
    cos_tab, sin_tab = rope_tables()

    def local_step(x, k_cache, v_cache, positions, att_ids, mlp_ids, norm_att, w_kv, router_att, w_query, w_out, norm_mlp, router_mlp, w_gate, w_up, w_down):
        flat = (TOK * SLOTS * HEADS, HD)
        wkv = w_kv.reshape(HID, HEADS, 2, HD).transpose(0, 2, 1, 3).reshape(HID * 2 * HEADS, HD)
        k_out, v_out, o, meta = attention_call(
            x, norm_att[None, :], wkv, router_att.T, w_query, k_cache.reshape(flat), v_cache.reshape(flat), att_ids.T, positions[None, :],
            jnp.asarray(cos_tab), jnp.asarray(sin_tab))
        xm = project_call(x, o, meta, w_out)
        y = experts_call(xm, norm_mlp[None, :], router_mlp.T, mlp_ids.T, w_gate, w_up, w_down)
        x_out = sum_call(xm, y)
        return x_out, k_out.reshape(k_cache.shape), v_out.reshape(v_cache.shape)

    token_spec = P('dp', None)
    cache_spec = P('dp', None, 'tp', None)
    expert_spec = P('tp', None, None)
    in_specs = (token_spec, cache_spec, cache_spec, P('dp'), token_spec, token_spec, P(), P(None, 'tp', None), P(), P(None, None, 'tp'), P(None, 'tp', None), P(), P(), expert_spec, expert_spec, expert_spec)
    out_specs = (token_spec, cache_spec, cache_spec)
    return jax.shard_map(local_step, mesh=mesh, in_specs=in_specs, out_specs=out_specs, check_vma=False)
```
